8 devices in a mesh: rep: 2 (over y, z), dp: 4 (over x, core).
Axes of the slice: x: 2, y: 2, z: 1, core: 2. Of those that a mesh axis runs over, the one named last changes fastest.
Arguments:
- x: bfloat16 [8, 2048, 1280], P(('rep', 'dp')), parts along dimension 0
- dy: bfloat16 [8, 2048, 1280], P(('rep', 'dp')), parts along dimension 0
- w_gate: bfloat16 [2, 1280, 4480], replicated
- w_up: bfloat16 [2, 1280, 4480], replicated
- w_down: bfloat16 [2, 4480, 1280], replicated
- m_w_gate: float32 [2, 1280, 4480], P(None, 'dp')
- m_w_up: float32 [2, 1280, 4480], P(None, 'dp')
- m_w_down: float32 [2, 4480, 1280], P(None, 'dp')
- v_w_gate: float32 [2, 1280, 4480], P(None, 'dp')
- v_w_up: float32 [2, 1280, 4480], P(None, 'dp')
- v_w_down: float32 [2, 4480, 1280], P(None, 'dp')
Outputs:
- output 1: bfloat16 [4, 1280, 4480], P('rep'), parts along dimension 0
- output 2: bfloat16 [4, 1280, 4480], P('rep'), parts along dimension 0
- output 3: bfloat16 [4, 4480, 1280], P('rep'), parts along dimension 0
- output 4: float32 [4, 1280, 4480], P('rep', 'dp'), parts along dimension 0
- output 5: float32 [4, 1280, 4480], P('rep', 'dp'), parts along dimension 0
- output 6: float32 [4, 4480, 1280], P('rep', 'dp'), parts along dimension 0
- output 7: float32 [4, 1280, 4480], P('rep', 'dp'), parts along dimension 0
- output 8: float32 [4, 1280, 4480], P('rep', 'dp'), parts along dimension 0
- output 9: float32 [4, 4480, 1280], P('rep', 'dp'), parts along dimension 0
There are 2 independent parts. The reference program is written for one: setup_inputs(seed, part) draws one part's arguments, and reference() takes and returns one part's arrays. A program takes and returns all parts, laid end to end along the dimension named above; an argument that names none is the same for every part.
All inputs are finite; a program needn't handle non-finite values.
Results may differ from the reference program's by a relative error of at most 0.022.
Values are sent between devices in bfloat16 or wider.
A program may use at most 2 GiB of HBM per device.

```python
import jax
import jax.numpy as jnp
from jax import lax

SEQUENCES = 4
TOKENS = 2048
D = 1280
FF = 4480
LAYERS = 2
NAMES = ("w_gate", "w_up", "w_down")
SHAPES = {"w_gate": (LAYERS, D, FF), "w_up": (LAYERS, D, FF), "w_down": (LAYERS, FF, D)}


def bump(key, n, height):
    away = (jnp.arange(n, dtype=jnp.int32) - jax.random.randint(key, (), 0, n, jnp.int32)) % n
    return jnp.where(away < n // 8, height, 1.0)


def together(key, own, strength):
    shared = jax.random.normal(key, own.shape[1:], jnp.float32)
    return (own + strength * shared) * lax.rsqrt(1 + strength * strength)


def setup_inputs(seed: int = 0, part: int = 0) -> dict:
    kx, kdy, ka, kb, kz, kf, kh, kl, *keys = jax.random.split(jax.random.key(seed), 8 + 3 * len(NAMES))
    kx, kdy, ka, kb = (jax.random.fold_in(k, part) for k in (kx, kdy, ka, kb))
    kw, km, kv = (keys[i::3] for i in range(3))
    shape = (SEQUENCES, TOKENS, D)
    much_x, much_dy = jax.random.uniform(kz, (2,), jnp.float32, 0.0, 1.0)
    loud = 2.0 ** jax.random.uniform(jax.random.fold_in(kz, 1), (), jnp.float32, -1.0, 2.0)
    layers = 2.0 ** jax.random.uniform(kl, (LAYERS, 1, 1), jnp.float32, -1.0, 1.0)
    x = together(ka, jax.random.normal(kx, shape, jnp.float32), much_x) * bump(kf, D, 4.0)
    dy = together(kb, jax.random.normal(kdy, shape, jnp.float32), much_dy)
    drawn = {"x": x.astype(jnp.bfloat16), "dy": (loud * dy * (SEQUENCES * TOKENS) ** -0.5).astype(jnp.bfloat16)}
    for key, name in zip(kw, NAMES, strict=True):
        w = jax.random.normal(key, SHAPES[name], jnp.float32) * SHAPES[name][1] ** -0.5
        drawn[name] = (w * {"w_gate": 1.0, "w_up": bump(kh, FF, 4.0), "w_down": layers}[name]).astype(jnp.bfloat16)
    for key, name in zip(km, NAMES, strict=True):
        drawn[f"m_{name}"] = 0.1 * jax.random.normal(key, SHAPES[name], jnp.float32)
    for key, name in zip(kv, NAMES, strict=True):
        drawn[f"v_{name}"] = jax.random.uniform(key, SHAPES[name], jnp.float32, 0.005, 0.015)
    return drawn


def matmul(a, w):
    return jnp.dot(a, w, preferred_element_type=jnp.float32).astype(jnp.bfloat16)


def normed(h):
    wide = h.astype(jnp.float32)
    scale = lax.rsqrt(jnp.mean(wide**2, -1, keepdims=True) + 1e-6)
    return (wide * scale).astype(jnp.bfloat16)


def layer(h, w):
    a = normed(h)
    gate = jnp.dot(a, w["w_gate"], preferred_element_type=jnp.float32)
    up = jnp.dot(a, w["w_up"], preferred_element_type=jnp.float32)
    return h + matmul((jax.nn.silu(gate) * up).astype(jnp.bfloat16), w["w_down"])


def adamw(w, m, v, g):
    m = 0.9 * m + 0.1 * g
    v = 0.95 * v + 0.05 * g * g
    step = m * lax.rsqrt(v + 1e-8) + 0.1 * w
    return (w - 0.02 * step).astype(jnp.bfloat16), m, v


def clipped(gradients, sum_of_squares, count):
    factor = jnp.minimum(1.0, 0.5 * lax.rsqrt(sum_of_squares / count + 1e-30))
    return [g * factor for g in gradients]


def stack(weights, h):
    return lax.scan(lambda h, w: (layer(h, w), None), h, weights)[0]


def reference(x, dy, w_gate, w_up, w_down, m_w_gate, m_w_up, m_w_down, v_w_gate, v_w_up, v_w_down):
    weights = dict(zip(NAMES, (w_gate, w_up, w_down), strict=True))

    def take(so_far, sequence):
        h, by_y = sequence
        _, back = jax.vjp(lambda w: stack(w, h), weights)
        return jax.tree.map(lambda total, term: total + term.astype(jnp.float32), so_far, back(by_y)[0]), None

    none_yet = {name: jnp.zeros(w.shape, jnp.float32) for name, w in weights.items()}
    by_weights, _ = lax.scan(take, none_yet, (x, dy))
    gradients = [by_weights[name].astype(jnp.bfloat16).astype(jnp.float32) for name in NAMES]
    gradients = clipped(gradients, sum(jnp.sum(g * g) for g in gradients), sum(g.size for g in gradients))
    new = [
        adamw(w.astype(jnp.float32), m, v, g)
        for w, m, v, g in zip((w_gate, w_up, w_down), (m_w_gate, m_w_up, m_w_down), (v_w_gate, v_w_up, v_w_down), gradients, strict=True)
    ]
    return tuple(one[which] for which in range(3) for one in new)
```

```python
import functools

import jax
import jax.numpy as jnp
from jax import lax
from jax.experimental import pallas as pl
from jax.experimental.pallas import tpu as pltpu
from jax.sharding import PartitionSpec as P

BF, F32 = jnp.bfloat16, jnp.float32
NN = (((1,), (0,)), ((), ()))
NT = (((1,), (1,)), ((), ()))
TN = (((0,), (0,)), ((), ()))
MIB = 2**20


def dot(a, b, dims):
    return lax.dot_general(a, b, dims, preferred_element_type=F32)


def params(mib=60):
    return pltpu.CompilerParams(vmem_limit_bytes=mib * MIB)


def cost(flops, nbytes):
    return pl.CostEstimate(flops=int(flops), bytes_accessed=int(nbytes), transcendentals=0)


def out(shape, dtype=BF):
    return jax.ShapeDtypeStruct(shape, dtype)


def normed_columns(h):
    wide = h.astype(F32)
    scale = lax.rsqrt(jnp.mean(wide * wide, 0, keepdims=True) + 1e-6)
    return (wide * scale).astype(BF)


def first_kernel(x, wg, wu, a_out, hid, s_out, q_out, a):
    @pl.when(pl.program_id(1) == 0)
    def _():
        wide = x[...].astype(F32)
        scale = lax.rsqrt(jnp.mean(wide * wide, -1, keepdims=True) + 1e-6)
        a[...] = (wide * scale).astype(BF).T
        a_out[...] = a[...]

    gate, up = dot(wg[...], a[...], TN), dot(wu[...], a[...], TN)
    sig = jax.nn.sigmoid(gate)
    silu = gate * sig
    hid[...] = (silu * up).astype(BF)
    s_out[...] = silu
    q_out[...] = up * (sig + silu * (1 - sig))


def first(x, w_gate, w_up):
    t, d = x.shape
    f = w_gate.shape[2]
    bt, bf = 1024, 640
    wide = pl.BlockSpec((bf, bt), lambda i, j: (j, i))
    weight = pl.BlockSpec((None, d, bf), lambda i, j: (0, 0, j))
    return pl.pallas_call(
        first_kernel,
        grid=(t // bt, f // bf),
        in_specs=[pl.BlockSpec((bt, d), lambda i, j: (i, 0)), weight, weight],
        out_specs=[pl.BlockSpec((d, bt), lambda i, j: (0, i)), wide, wide, wide],
        out_shape=[out((d, t)), out((f, t)), out((f, t), F32), out((f, t), F32)],
        scratch_shapes=[pltpu.VMEM((d, bt), BF)],
        compiler_params=params(),
        cost_estimate=cost(4 * t * d * f, 130e6),
        name="first",
    )(x, w_gate, w_up)


def down_kernel(w, hid, x, h):
    h[...] = x[...].T + dot(w[...], hid[...], TN).astype(BF)


def down(w_down, hid, x):
    t, d = x.shape
    f = hid.shape[0]
    bt = 512
    return pl.pallas_call(
        down_kernel,
        grid=(t // bt,),
        in_specs=[
            pl.BlockSpec((None, f, d), lambda i: (0, 0, 0), pipeline_mode=pl.Buffered(1)),
            pl.BlockSpec((f, bt), lambda i: (0, i)),
            pl.BlockSpec((bt, d), lambda i: (i, 0)),
        ],
        out_specs=pl.BlockSpec((d, bt), lambda i: (0, i)),
        out_shape=out((d, t)),
        compiler_params=params(),
        cost_estimate=cost(2 * t * d * f, 40e6),
        name="down",
    )(w_down, hid, x)


def second_kernel(h, dy, wg, wu, wd, a_out, hid, dgate, dup, a):
    @pl.when(pl.program_id(1) == 0)
    def _():
        a[...] = normed_columns(h[...])
        a_out[...] = a[...]

    gate, up = dot(wg[...], a[...], TN), dot(wu[...], a[...], TN)
    back = dot(wd[...], dy[...], NT).astype(BF).astype(F32)
    sig = jax.nn.sigmoid(gate)
    silu = gate * sig
    hid[...] = (silu * up).astype(BF)
    dup[...] = (back * silu).astype(BF)
    dgate[...] = (back * (up * (sig + silu * (1 - sig)))).astype(BF)


def second(h, dy, w_gate, w_up, w_down):
    d, t = h.shape
    f = w_gate.shape[2]
    bt, bf = 1024, 640
    wide = pl.BlockSpec((bf, bt), lambda i, j: (j, i))
    weight = pl.BlockSpec((None, d, bf), lambda i, j: (1, 0, j))
    return pl.pallas_call(
        second_kernel,
        grid=(t // bt, f // bf),
        in_specs=[
            pl.BlockSpec((d, bt), lambda i, j: (0, i)),
            pl.BlockSpec((bt, d), lambda i, j: (i, 0)),
            weight,
            weight,
            pl.BlockSpec((None, bf, d), lambda i, j: (1, j, 0)),
        ],
        out_specs=[pl.BlockSpec((d, bt), lambda i, j: (0, i)), wide, wide, wide],
        out_shape=[out((d, t)), out((f, t)), out((f, t)), out((f, t))],
        scratch_shapes=[pltpu.VMEM((d, bt), BF)],
        compiler_params=params(),
        cost_estimate=cost(6 * t * d * f, 130e6),
        name="second",
    )(h, dy, w_gate, w_up, w_down)


def back_kernel(wg, wu, dgate, dup, h, dy, d_out, da):
    j, rows = pl.program_id(1), wg.shape[0]
    part = dot(wg[...], dgate[...], NN).astype(BF) + dot(wu[...], dup[...], NN).astype(BF)
    da[pl.ds(pl.multiple_of(j * rows, rows), rows), :] = part

    @pl.when(j == pl.num_programs(1) - 1)
    def _():
        wide, up = h[...].astype(F32), da[...].astype(F32)
        scale = lax.rsqrt(jnp.mean(wide * wide, 0, keepdims=True) + 1e-6)
        along = jnp.mean(up * wide, 0, keepdims=True) * (scale * scale * scale)
        d_out[...] = dy[...].T + (up * scale - wide * along).astype(BF)


def back(w_gate, w_up, dgate, dup, h, dy):
    f, t = dgate.shape
    d = h.shape[0]
    bt, bm = 512, 640
    weight = pl.BlockSpec((None, bm, f), lambda i, j: (1, j, 0))
    wide = pl.BlockSpec((f, bt), lambda i, j: (0, i))
    return pl.pallas_call(
        back_kernel,
        grid=(t // bt, d // bm),
        in_specs=[weight, weight, wide, wide, pl.BlockSpec((d, bt), lambda i, j: (0, i)), pl.BlockSpec((bt, d), lambda i, j: (i, 0))],
        out_specs=pl.BlockSpec((d, bt), lambda i, j: (0, i)),
        out_shape=out((d, t)),
        scratch_shapes=[pltpu.VMEM((d, bt), BF)],
        compiler_params=params(),
        cost_estimate=cost(4 * t * d * f, 130e6),
        name="back",
    )(w_gate, w_up, dgate, dup, h, dy)


def hidden_back_kernel(w, d, s, q, dgate, dup):
    back = dot(w[...], d[...], NN).astype(BF).astype(F32)
    dup[...] = (back * s[...]).astype(BF)
    dgate[...] = (back * q[...]).astype(BF)


def hidden_back(w_down, d_h, s, q):
    d, t = d_h.shape
    f = s.shape[0]
    bt, bf = 1024, 640
    wide = pl.BlockSpec((bf, bt), lambda i, j: (j, i))
    return pl.pallas_call(
        hidden_back_kernel,
        grid=(t // bt, f // bf),
        in_specs=[pl.BlockSpec((None, bf, d), lambda i, j: (0, j, 0)), pl.BlockSpec((d, bt), lambda i, j: (0, i)), wide, wide],
        out_specs=[wide, wide],
        out_shape=[out((f, t)), out((f, t))],
        compiler_params=params(),
        cost_estimate=cost(2 * t * d * f, 130e6),
        name="hidden_back",
    )(w_down, d_h, s, q)


def grad_kernel(at, *refs, terms, dims, add, whole):
    operands, rest = refs[: 2 * terms], refs[2 * terms :]
    total = sum(
        (dot(left[...].reshape(-1, left.shape[-1]), right[...], dims) for left, right in zip(operands[::2], operands[1::2], strict=True)),
        start=jnp.zeros((), F32) if add is None else 0,
    )
    if add is not None:
        total = total + rest[0][...].reshape(total.shape).astype(F32)
        rest = rest[1:]
    for o, dtype in zip(rest, whole, strict=True):
        o[...] = total.reshape(o.shape).astype(dtype)


def grad_wide(at, pairs, block, received=None, dtype=BF, bn=1536):
    rows, t = pairs[0][0].shape[1:]
    f = pairs[0][1].shape[0]
    in_specs, operands = [], []
    for left, right in pairs:
        in_specs += [
            pl.BlockSpec((None, rows, t), lambda j, at: (block(at), 0, 0)),
            pl.BlockSpec((bn, t), lambda j, at: (j, 0)),
        ]
        operands += [left, right]
    if received is not None:
        which, array = received
        in_specs.append(pl.BlockSpec((None, rows, bn), lambda j, at: (which, 0, j)))
        operands.append(array)
    return pl.pallas_call(
        functools.partial(grad_kernel, terms=len(pairs), dims=NT, add=received, whole=(dtype,)),
        grid_spec=pltpu.PrefetchScalarGridSpec(
            num_scalar_prefetch=1,
            grid=(pl.cdiv(f, bn),),
            in_specs=in_specs,
            out_specs=[pl.BlockSpec((rows, bn), lambda j, at: (0, j))],
        ),
        out_shape=[out((rows, f), dtype)],
        compiler_params=params(),
        cost_estimate=cost(2 * rows * t * f * len(pairs), 30e6),
        name="grad_wide",
    )(at, *operands)[0]


def grad_tall(at, pairs, block, dims, received=None, dtype=BF):
    rows, t = pairs[0][0].shape[1:]
    d = pairs[0][1].shape[1 - dims[0][1][0]]
    bm = rows // 2
    in_specs, operands = [], []
    for left, right in pairs:
        in_specs += [
            pl.BlockSpec((None, bm, t), lambda j, at: (block(at), j, 0)),
            pl.BlockSpec(right.shape, lambda j, at: (0, 0)),
        ]
        operands += [left, right]
    if received is not None:
        which, array = received
        in_specs.append(pl.BlockSpec((None, bm, d), lambda j, at: (which, j, 0)))
        operands.append(array)
    return pl.pallas_call(
        functools.partial(grad_kernel, terms=len(pairs), dims=dims, add=received, whole=(dtype,)),
        grid_spec=pltpu.PrefetchScalarGridSpec(
            num_scalar_prefetch=1,
            grid=(rows // bm,),
            in_specs=in_specs,
            out_specs=[pl.BlockSpec((bm, d), lambda j, at: (j, 0))],
        ),
        out_shape=[out((rows, d), dtype)],
        compiler_params=params(),
        cost_estimate=cost(2 * rows * t * d * len(pairs), 30e6),
        name="grad_tall",
    )(at, *operands)[0]


def adam_kernel(at, factor, *refs, parts):
    grads, (w, m, v) = refs[:parts], refs[parts : parts + 3]
    w_out, m_out, v_out = refs[-3:]
    g = grads[0][...].astype(F32)
    if parts == 2:
        g = (g + grads[1][...].astype(F32)).astype(BF).astype(F32)
    g = g * factor[0]
    m_new = 0.9 * m[...] + 0.1 * g
    v_new = 0.95 * v[...] + 0.05 * g * g
    wide = w[...].astype(F32)
    w_out[...] = (wide - 0.02 * (m_new * lax.rsqrt(v_new + 1e-8) + 0.1 * wide)).astype(BF)
    m_out[...] = m_new
    v_out[...] = v_new


def adam(at, factor, layer, grads, w, m, v, before):
    rows, cols = grads[0].shape
    br = rows // 5
    n = rows // br
    own = pl.BlockSpec((None, br, cols), lambda i, at: (layer, i, 0))
    flat = pl.BlockSpec((br, cols), lambda i, at: (i, 0))
    in_specs = [pl.BlockSpec(memory_space=pltpu.SMEM)] + [flat] * len(grads)
    in_specs += [pl.BlockSpec((None, br, cols), lambda i, at: (layer, (2 * at[0] + at[1]) * n + i, 0)), own, own]
    operands = [factor, *grads, w, m, v]
    aliases = {}
    if before is not None:
        aliases = {1 + len(operands): 1, 2 + len(operands): 2}
        operands += before
        in_specs += [pl.BlockSpec(memory_space=pl.ANY)] * 2
    return pl.pallas_call(
        functools.partial(adam_kernel, parts=len(grads)),
        grid_spec=pltpu.PrefetchScalarGridSpec(num_scalar_prefetch=1, grid=(n,), in_specs=in_specs, out_specs=[flat, own, own]),
        out_shape=[out((rows, cols)), out(m.shape, F32), out(v.shape, F32)],
        input_output_aliases=aliases,
        compiler_params=params(),
        cost_estimate=cost(1e9, 31e6),
        name="adam",
    )(at, *operands)


def place_kernel(at, *refs):
    o = refs[-1]
    i = pl.program_id(0)
    for n in range(4):

        @pl.when(i == n)
        def _(n=n):
            o[...] = refs[n][...]


def place(at, layer, blocks, shape, before):
    rows, cols = blocks[0].shape
    br = rows // 5

    def spec(n):
        return pl.BlockSpec((br, cols), lambda i, j, at: (jnp.where(i < n, 0, jnp.where(i > n, 4, j)), 0))

    def where(i, j, at):
        x = jnp.where(i < 2, at[0], 1 - at[0])
        c = jnp.where(i % 2 == 0, at[1], 1 - at[1])
        return layer, (2 * x + c) * 5 + j, 0

    in_specs, operands, aliases = [spec(n) for n in range(4)], list(blocks), {}
    if before is not None:
        aliases = {5: 0}
        in_specs.append(pl.BlockSpec(memory_space=pl.ANY))
        operands.append(before)
    return pl.pallas_call(
        place_kernel,
        grid_spec=pltpu.PrefetchScalarGridSpec(
            num_scalar_prefetch=1, grid=(4, 5), in_specs=in_specs, out_specs=pl.BlockSpec((None, br, cols), where)
        ),
        out_shape=out(shape),
        input_output_aliases=aliases,
        compiler_params=params(32),
        cost_estimate=cost(1e9, 23e6),
        name="place",
    )(at, *operands)


def sum_kernel(*refs, parts):
    grads, o = refs[:-1], refs[-1]

    @pl.when(pl.program_id(0) == 0)
    def _():
        o[...] = jnp.zeros_like(o)

    g = grads[0][...].astype(F32)
    if parts == 2:
        g = (g + grads[1][...].astype(F32)).astype(BF).astype(F32)
    g = g * g
    o[...] += jnp.sum(g.reshape(-1, 8, g.shape[1]), 0)


def sum_of_squares(grads):
    rows, cols = grads[0].shape
    br = rows // 5
    total = pl.pallas_call(
        functools.partial(sum_kernel, parts=len(grads)),
        grid=(5,),
        in_specs=[pl.BlockSpec((br, cols), lambda i: (i, 0))] * len(grads),
        out_specs=pl.BlockSpec((8, cols), lambda i: (0, 0)),
        out_shape=out((8, cols), F32),
        compiler_params=params(32),
        cost_estimate=cost(1e8, 9e6),
        name="sum_of_squares",
    )(*grads)
    return jnp.sum(total)


def after(value, *others):
    return lax.optimization_barrier((value, *others))[0]


ACROSS = [(0, 2), (2, 0), (1, 3), (3, 1)]
SIBLING = [(0, 1), (1, 0), (2, 3), (3, 2)]


def across(a):
    return lax.ppermute(a, "dp", ACROSS)


def sibling(a):
    return lax.ppermute(a, "dp", SIBLING)


def step(x, dy, w_gate, w_up, w_down, m_gate, m_up, m_down, v_gate, v_up, v_down):
    dp = lax.axis_index("dp")
    at = jnp.stack([dp // 2, dp % 2]).astype(jnp.int32)
    x, dy = x[0], dy[0]
    t, d = x.shape
    f = w_gate.shape[2]

    dy_far = across(dy)
    a1, hid1, s1, q1 = first(x, w_gate, w_up)
    h1 = down(w_down, hid1, x)
    h1_far = across(h1)
    a2, hid2, dgate2, dup2 = second(h1, dy, w_gate, w_up, w_down)
    d1 = back(w_gate, w_up, dgate2, dup2, h1, dy)

    def blocks(a):
        return a.reshape(4, a.shape[0] // 4, a.shape[1])

    peer = lambda core: lambda at: 2 * (1 - at[0]) + (at[1] if core else 1 - at[1])
    same = lambda core: lambda at: 2 * at[0] + (at[1] if core else 1 - at[1])

    def layer1(grad, pairs, **kw):
        theirs = jnp.stack([grad(at, pairs, peer(False), **kw), grad(at, pairs, same(False), **kw)])
        got = sibling(theirs)

        def finish():
            send = grad(at, pairs, peer(True), received=(0, got), **kw)
            far = across(send)
            keep = grad(at, pairs, same(True), received=(1, got), dtype=F32, **kw)
            return keep, far

        return finish

    fin_down = layer1(grad_tall, [(blocks(hid1), d1)], dims=NT)
    dgate1, dup1 = hidden_back(w_down, d1, s1, q1)
    g_down1 = fin_down()
    fin_gate = layer1(grad_wide, [(blocks(a1), dgate1)])
    fin_up = layer1(grad_wide, [(blocks(a1), dup1)])
    g_gate1, g_up1 = fin_gate(), fin_up()

    h1_far = after(h1_far, g_gate1[0], g_up1[0])
    a2f, hid2f, dgate2f, dup2f = second(h1_far, dy_far, w_gate, w_up, w_down)

    def layer2(grad, pairs, **kw):
        theirs = grad(at, pairs, same(False), **kw)
        got = sibling(theirs)
        return lambda: grad(at, pairs, same(True), received=(0, got[None]), **kw)

    wide = lambda own, far: [(blocks(a2), own), (blocks(a2f), far)]
    fin_down = layer2(grad_tall, [(blocks(hid2), dy), (blocks(hid2f), dy_far)], dims=NN)
    fin_gate = layer2(grad_wide, wide(dgate2, dgate2f), bn=768)
    fin_up = layer2(grad_wide, wide(dup2, dup2f), bn=768)
    g_down2, g_gate2, g_up2 = fin_down(), fin_gate(), fin_up()

    grads = [[g_gate1, (g_gate2,)], [g_up1, (g_up2,)], [g_down1, (g_down2,)]]
    squares = sum(sum_of_squares(g) for both in grads for g in both)
    squares = lax.psum(squares, "dp")
    count = 3 * 2 * d * f
    factor = jnp.minimum(1.0, 0.5 * lax.rsqrt(squares / count + 1e-30)).reshape(1)

    new_w, new_m, new_v = [], [], []
    for both, w, m, v in zip(grads, (w_gate, w_up, w_down), (m_gate, m_up, m_down), (v_gate, v_up, v_down), strict=True):
        moments, placed = None, None
        for layer, g in enumerate(both):
            own, *moments = adam(at, factor, layer, g, w, m, v, moments)
            far = across(own)
            placed = place(at, layer, (own, sibling(own), far, sibling(far)), w.shape, placed)
        new_w.append(placed)
        new_m.append(moments[0])
        new_v.append(moments[1])
    return (*new_w, *new_m, *new_v)


def solution(mesh):
    tokens, whole, rows = P(("rep", "dp")), P(), P(None, "dp")
    return jax.shard_map(
        step,
        mesh=mesh,
        in_specs=(tokens,) * 2 + (whole,) * 3 + (rows,) * 6,
        out_specs=(P("rep"),) * 3 + (P("rep", "dp"),) * 6,
        check_vma=False,
    )
```

```python
import functools

import jax
import jax.numpy as jnp
from jax import lax
from jax.experimental import pallas as pl
from jax.experimental.pallas import tpu as pltpu
from jax.sharding import PartitionSpec as P

BF, F32 = jnp.bfloat16, jnp.float32
NN = (((1,), (0,)), ((), ()))
NT = (((1,), (1,)), ((), ()))
CHUNK = 256
TOKENS, UNITS = 1024, 512


def dot(a, b, dims):
    return lax.dot_general(a, b, dims, preferred_element_type=F32)


def params():
    return pltpu.CompilerParams(vmem_limit_bytes=61 * 2**20)


def cost(flops, nbytes):
    return pl.CostEstimate(flops=int(flops), bytes_accessed=int(nbytes), transcendentals=0)


def out(shape, dtype=BF):
    return jax.ShapeDtypeStruct(shape, dtype)


def once(shape, index):
    return pl.BlockSpec(shape, index, pipeline_mode=pl.Buffered(1))


def sigmoid(x):
    return 0.5 * jnp.tanh(0.5 * x) + 0.5


def chunks(n, size=CHUNK):
    return [slice(at, min(at + size, n)) for at in range(0, n, size)]


def norm(h, a, a_out):
    for r in chunks(a.shape[0]):
        wide = h[r, :].astype(F32)
        scale = lax.rsqrt(jnp.mean(wide * wide, -1, keepdims=True) + 1e-6)
        a[r, :] = (wide * scale).astype(BF)
        a_out[:, r] = a[r, :].T


def at_steps(tile, whole, last_units):
    j, last = pl.program_id(1), pl.num_programs(1) - 1
    pl.when(j < last)(lambda: tile(whole, False))
    pl.when(j == last)(lambda: tile(last_units, True))


def first_kernel(x, wg, wu, wd, a_out, hid, s_out, q_out, h_out, a, units, total, *, last_units):
    @pl.when(pl.program_id(1) == 0)
    def _():
        norm(x, a, a_out)
        total[...] = jnp.zeros_like(total)

    def tile(n, end):
        for c in chunks(n):
            gate, up = dot(a[...], wg[:, c], NN), dot(a[...], wu[:, c], NN)
            sig = sigmoid(gate)
            silu = gate * sig
            units[:, c] = (silu * up).astype(BF)
            hid[c, :] = units[:, c].T
            s_out[:, c] = silu
            q_out[:, c] = up * (sig + silu * (1 - sig))
        for c in chunks(total.shape[1]):
            part = total[:, c] + dot(units[:, :n], wd[:n, c], NN)
            if end:
                h_out[:, c] = x[:, c] + part.astype(BF)
            else:
                total[:, c] = part

    at_steps(tile, hid.shape[0], last_units)


def first(x, w_gate, w_up, w_down):
    t, d = x.shape
    f = w_gate.shape[2]
    n = pl.cdiv(f, UNITS)
    wide = pl.BlockSpec((TOKENS, UNITS), lambda i, j: (i, j))
    weight = pl.BlockSpec((None, d, UNITS), lambda i, j: (0, 0, j))
    state = pl.BlockSpec((TOKENS, d), lambda i, j: (i, 0))
    return pl.pallas_call(
        functools.partial(first_kernel, last_units=f - (n - 1) * UNITS),
        grid=(t // TOKENS, n),
        in_specs=[state, weight, weight, pl.BlockSpec((None, UNITS, d), lambda i, j: (0, j, 0))],
        out_specs=[pl.BlockSpec((d, TOKENS), lambda i, j: (0, i)), pl.BlockSpec((UNITS, TOKENS), lambda i, j: (j, i)), wide, wide, state],
        out_shape=[out((d, t)), out((f, t)), out((t, f), F32), out((t, f), F32), out((t, d))],
        scratch_shapes=[pltpu.VMEM((TOKENS, d), BF), pltpu.VMEM((TOKENS, UNITS), BF), pltpu.VMEM((TOKENS, d), F32)],
        compiler_params=params(),
        cost_estimate=cost(6 * t * d * f, 170e6),
        name="first",
    )(x, w_gate, w_up, w_down)


def second_units(a, dy, wg, wu, wd, hid, dgu, n):
    for c in chunks(n):
        gate, up = dot(a[...], wg[:, c], NN), dot(a[...], wu[:, c], NN)
        back = dot(dy[...], wd[c, :], NT).astype(BF).astype(F32)
        sig = sigmoid(gate)
        silu = gate * sig
        hid[c, :] = (silu * up).astype(BF).T
        dgu[0, :, c] = (back * (up * (sig + silu * (1 - sig)))).astype(BF)
        dgu[1, :, c] = (back * silu).astype(BF)


def second_kernel(h, dy, wg, wu, wd, a_out, hid, dgu, a, *, last_units):
    @pl.when(pl.program_id(1) == 0)
    def _():
        norm(h, a, a_out)

    at_steps(lambda n, end: second_units(a, dy, wg, wu, wd, hid, dgu, n), hid.shape[0], last_units)


def second(h, dy, w_gate, w_up, w_down):
    t, d = h.shape
    f = w_gate.shape[2]
    n = pl.cdiv(f, UNITS)
    weight = pl.BlockSpec((None, d, UNITS), lambda i, j: (1, 0, j))
    state = pl.BlockSpec((TOKENS, d), lambda i, j: (i, 0))
    return pl.pallas_call(
        functools.partial(second_kernel, last_units=f - (n - 1) * UNITS),
        grid=(t // TOKENS, n),
        in_specs=[state, state, weight, weight, pl.BlockSpec((None, UNITS, d), lambda i, j: (1, j, 0))],
        out_specs=[
            pl.BlockSpec((d, TOKENS), lambda i, j: (0, i)),
            pl.BlockSpec((UNITS, TOKENS), lambda i, j: (j, i)),
            pl.BlockSpec((2, TOKENS, UNITS), lambda i, j: (0, i, j)),
        ],
        out_shape=[out((d, t)), out((f, t)), out((2, t, f))],
        scratch_shapes=[pltpu.VMEM((TOKENS, d), BF)],
        compiler_params=params(),
        cost_estimate=cost(6 * t * d * f, 130e6),
        name="second",
    )(h, dy, w_gate, w_up, w_down)


def second_back_kernel(h, dy, wg, wu, wd, a_out, hid, dgu, d_out, a, of_gate, of_up, *, last_units):
    @pl.when(pl.program_id(1) == 0)
    def _():
        norm(h, a, a_out)
        of_gate[...] = jnp.zeros_like(of_gate)
        of_up[...] = jnp.zeros_like(of_up)

    def tile(n, end):
        second_units(a, dy, wg, wu, wd, hid, dgu, n)
        for c in chunks(of_gate.shape[1]):
            gates = of_gate[:, c] + dot(dgu[0, :, :n], wg[c, :n], NT)
            ups = of_up[:, c] + dot(dgu[1, :, :n], wu[c, :n], NT)
            if end:
                of_gate[:, c] = (gates.astype(BF) + ups.astype(BF)).astype(F32)
            else:
                of_gate[:, c], of_up[:, c] = gates, ups
        if end:
            for r in chunks(of_gate.shape[0]):
                da, wide = of_gate[r, :], h[r, :].astype(F32)
                scale = lax.rsqrt(jnp.mean(wide * wide, -1, keepdims=True) + 1e-6)
                along = jnp.mean(da * wide, -1, keepdims=True) * (scale * scale * scale)
                d_out[r, :] = dy[r, :] + (da * scale - wide * along).astype(BF)

    at_steps(tile, hid.shape[0], last_units)


def second_back(h, dy, w_gate, w_up, w_down):
    t, d = h.shape
    f = w_gate.shape[2]
    n = pl.cdiv(f, UNITS)
    weight = pl.BlockSpec((None, d, UNITS), lambda i, j: (1, 0, j))
    state = pl.BlockSpec((TOKENS, d), lambda i, j: (i, 0))
    return pl.pallas_call(
        functools.partial(second_back_kernel, last_units=f - (n - 1) * UNITS),
        grid=(t // TOKENS, n),
        in_specs=[state, state, weight, weight, pl.BlockSpec((None, UNITS, d), lambda i, j: (1, j, 0))],
        out_specs=[
            pl.BlockSpec((d, TOKENS), lambda i, j: (0, i)),
            pl.BlockSpec((UNITS, TOKENS), lambda i, j: (j, i)),
            pl.BlockSpec((2, TOKENS, UNITS), lambda i, j: (0, i, j)),
            state,
        ],
        out_shape=[out((d, t)), out((f, t)), out((2, t, f)), out((t, d))],
        scratch_shapes=[pltpu.VMEM((TOKENS, d), BF), pltpu.VMEM((TOKENS, d), F32), pltpu.VMEM((TOKENS, d), F32)],
        compiler_params=params(),
        cost_estimate=cost(10 * t * d * f, 130e6),
        name="second_back",
    )(h, dy, w_gate, w_up, w_down)


def on(x_same, core_same):
    def block(at):
        return 2 * (at[0] if x_same else 1 - at[0]) + (at[1] if core_same else 1 - at[1])

    return block


def call(kernel, at, grid, in_specs, out_specs, out_shape, operands, flops, nbytes, **kw):
    return pl.pallas_call(
        kernel,
        grid_spec=pltpu.PrefetchScalarGridSpec(num_scalar_prefetch=1, grid=grid, in_specs=in_specs, out_specs=out_specs),
        out_shape=out_shape,
        compiler_params=params(),
        cost_estimate=cost(flops, nbytes),
        **kw,
    )(at, *operands)


def hidden_back_kernel(at, w, d, s, q, hid, dgu, theirs):
    for c in chunks(w.shape[0]):
        back = dot(d[...], w[c, :], NT).astype(BF).astype(F32)
        dgu[1, :, c] = (back * s[:, c]).astype(BF)
        dgu[0, :, c] = (back * q[:, c]).astype(BF)

    @pl.when(pl.program_id(0) < pl.num_programs(0) - 1)
    def _():
        theirs[...] = dot(hid[...], d[...], NN).astype(BF)


def hidden_back(at, w_down, d_h, s, q, hid):
    t, d = d_h.shape
    f = s.shape[1]
    n = pl.cdiv(f, UNITS) - 1
    bg = f // (2 * n)
    wide = pl.BlockSpec((t, UNITS), lambda j, at: (0, j))
    hid = hid.reshape(4, n // 2, bg, t)

    def part(j, at):
        j = jnp.minimum(j, n - 1)
        return (jnp.where(j < n // 2, on(False, False)(at), on(True, False)(at)), j % (n // 2), 0, 0)

    dgu, theirs = call(
        hidden_back_kernel,
        at,
        (n + 1,),
        [
            pl.BlockSpec((None, UNITS, d), lambda j, at: (0, j, 0)),
            once((t, d), lambda j, at: (0, 0)),
            wide,
            wide,
            pl.BlockSpec((None, None, bg, t), part),
        ],
        [pl.BlockSpec((2, t, UNITS), lambda j, at: (0, 0, j)), pl.BlockSpec((None, bg, d), lambda j, at: (jnp.minimum(j, n - 1), 0, 0))],
        [out((2, t, f)), out((n, bg, d))],
        (w_down, d_h, s, q, hid),
        3 * t * d * f,
        150e6,
    )
    return dgu, theirs.reshape(2, f // 4, d)


def wide_kernel(at, *refs, terms, add):
    operands, rest = refs[: 3 * terms], refs[3 * terms :]
    rows = operands[0].shape[0]
    total = 0
    for one, two, right in zip(operands[::3], operands[1::3], operands[2::3], strict=True):
        total = total + dot(jnp.concatenate([one[...], two[...]], 0), right[...], NN)
    if add:
        got, send, keep = rest
        total = total + got[...].reshape(total.shape).astype(F32)
        send[...], keep[...] = total[:rows].astype(BF), total[rows:]
    elif terms == 2:
        send, keep = rest
        send[...], keep[...] = total[:rows].astype(BF), total[rows:]
    else:
        rest[0][...] = total.reshape(rest[0].shape).astype(BF)


def grad_wide(at, pairs, one, two, got=None, bn=1536, both=False):
    rows, t = pairs[0][0].shape[1:]
    f = pairs[0][1].shape[2]
    in_specs, operands = [], []
    for left, right in pairs:
        in_specs += [pl.BlockSpec((None, rows, t), lambda w, j, at, b=b: (b(at), 0, 0)) for b in (one, two)]
        in_specs.append(pl.BlockSpec((None, t, bn), lambda w, j, at: (w, 0, j)))
        operands += [left, left, right]
    pair = pl.BlockSpec((None, 2, rows, bn), lambda w, j, at: (w, 0, 0, j))
    single = pl.BlockSpec((None, rows, bn), lambda w, j, at: (w, 0, j))
    if got is not None:
        in_specs.append(pair)
        operands.append(got)
    if both:
        out_specs, shapes = [pair], [out((2, 2, rows, f))]
    else:
        out_specs, shapes = [single, single], [out((2, rows, f)), out((2, rows, f), F32)]
    return call(
        functools.partial(wide_kernel, terms=len(pairs), add=got is not None),
        at,
        (2, pl.cdiv(f, bn)),
        in_specs,
        out_specs,
        shapes,
        operands,
        8 * rows * t * f * len(pairs),
        60e6,
    )


def tall_kernel(at, *refs, terms, add):
    operands, rest = refs[: 2 * terms], refs[2 * terms :]
    total = 0
    for left, right in zip(operands[::2], operands[1::2], strict=True):
        total = total + dot(left[...], right[...], NN)
    if add:
        total = total + rest[0][...].astype(F32)
    send, keep = rest[-2:]
    half = pl.num_programs(0) // 2

    @pl.when(pl.program_id(0) < half)
    def _():
        send[...] = total.astype(BF)

    @pl.when(pl.program_id(0) >= half)
    def _():
        keep[...] = total


def grad_tall(at, pairs, one, two, got=None):
    rows, t = pairs[0][0].shape[1:]
    d = pairs[0][1].shape[1]
    half = 2
    bm = rows // half
    in_specs, operands = [], []
    for left, right in pairs:
        in_specs += [
            pl.BlockSpec((None, bm, t), lambda j, at: (jnp.where(j < half, one(at), two(at)), j % half, 0)),
            once(right.shape, lambda j, at: (0, 0)),
        ]
        operands += [left, right]
    if got is not None:
        in_specs.append(pl.BlockSpec((None, bm, d), lambda j, at: (j // half, j % half, 0)))
        operands.append(got)
    return call(
        functools.partial(tall_kernel, terms=len(pairs), add=got is not None),
        at,
        (2 * half,),
        in_specs,
        [pl.BlockSpec((bm, d), lambda j, at: (jnp.minimum(j, half - 1), 0)), pl.BlockSpec((bm, d), lambda j, at: (jnp.maximum(j - half, 0), 0))],
        [out((rows, d)), out((rows, d), F32)],
        operands,
        4 * rows * t * d * len(pairs),
        60e6,
    )


def squares_kernel(*refs):
    o = refs[-1]

    @pl.when(pl.program_id(0) == 0)
    def _():
        o[...] = jnp.zeros_like(o)

    total = o[...]
    for keep, far in zip(refs[:-1:2], refs[1:-1:2], strict=True):
        g = (keep[...] + far[...].astype(F32)).astype(BF).astype(F32)
        g = jnp.sum((g * g).reshape(-1, 8, g.shape[1]), 0)
        total = total + sum(g[:, c] for c in chunks(g.shape[1], 128))
    o[...] = total


def sum_of_squares(pairs):
    n = 5
    pairs = [a.reshape(-1, a.shape[-1]) for pair in pairs for a in pair]
    return pl.pallas_call(
        squares_kernel,
        grid=(n,),
        in_specs=[pl.BlockSpec((a.shape[0] // n, a.shape[1]), lambda i: (i, 0)) for a in pairs],
        out_specs=pl.BlockSpec((8, 128), lambda i: (0, 0)),
        out_shape=out((8, 128), F32),
        compiler_params=params(),
        cost_estimate=cost(1e9, 4e6 * len(pairs)),
        name="squares",
    )(*pairs)


UNITS_OF_ROWS = 5


def adam_kernel(at, factor, keep, far, w, m, v, *rest):
    w_out, m_out, v_out = rest[-3:]
    g = (keep[...] + far[...].astype(F32)).astype(BF).astype(F32) * factor[0]
    m_new = 0.9 * m[...] + 0.1 * g
    v_new = 0.95 * v[...] + 0.05 * g * g
    wide = w[...].astype(F32)
    w_out[...] = (wide - 0.02 * (m_new * lax.rsqrt(v_new + 1e-8) + 0.1 * wide)).astype(BF)
    m_out[...] = m_new
    v_out[...] = v_new


def adam(at, factor, layer, which, part, keep, far, w, m, v, before):
    rows, cols = keep.shape[1:]
    br = rows // UNITS_OF_ROWS
    low, high = part
    own = pl.BlockSpec((None, br, cols), lambda i, at: (layer, low + i, 0))
    grad = pl.BlockSpec((None, br, cols), lambda i, at: (which, low + i, 0))
    in_specs = [pl.BlockSpec(memory_space=pltpu.SMEM), grad, grad]
    in_specs += [pl.BlockSpec((None, br, cols), lambda i, at: (layer, (2 * at[0] + at[1]) * UNITS_OF_ROWS + low + i, 0)), own, own]
    operands = [factor, keep, far, w, m, v]
    aliases = {}
    if before is not None:
        aliases = {1 + len(operands): 1, 2 + len(operands): 2}
        operands += before
        in_specs += [pl.BlockSpec(memory_space=pl.ANY)] * 2
    return call(
        adam_kernel,
        at,
        (high - low,),
        in_specs,
        [pl.BlockSpec((br, cols), lambda i, at: (i, 0)), own, own],
        [out((br * (high - low), cols)), out(m.shape, F32), out(v.shape, F32)],
        operands,
        1e9,
        6e6 * (high - low),
        input_output_aliases=aliases,
    )


def place_kernel(at, *refs, count):
    for n in range(count):
        pl.when(pl.program_id(0) == n)(functools.partial(lambda n: refs[-1].__setitem__(..., refs[n][...]), n))


def place(at, layer, part, blocks, wheres, shape, before):
    low, high = part
    k = high - low
    cols = blocks[0].shape[1]
    br = blocks[0].shape[0] // k

    def spec(n):
        return pl.BlockSpec((br, cols), lambda i, j, at: (jnp.where(i < n, 0, jnp.where(i > n, k - 1, j)), 0))

    def where(i, j, at):
        b = wheres[0](at)
        for n, w in enumerate(wheres[1:], 1):
            b = jnp.where(i == n, w(at), b)
        return layer, b * UNITS_OF_ROWS + low + j, 0

    in_specs, operands, aliases = [spec(n) for n in range(len(blocks))], list(blocks), {}
    if before is not None:
        aliases = {1 + len(blocks): 0}
        in_specs.append(pl.BlockSpec(memory_space=pl.ANY))
        operands.append(before)
    return call(
        functools.partial(place_kernel, count=len(blocks)),
        at,
        (len(blocks), k),
        in_specs,
        pl.BlockSpec((None, br, cols), where),
        out(shape),
        operands,
        1e9,
        1.2e6 * k * len(blocks),
        input_output_aliases=aliases,
    )


def after(value, *others):
    return lax.optimization_barrier((value, *others))[0]


ACROSS = [(0, 2), (2, 0), (1, 3), (3, 1)]
SIBLING = [(0, 1), (1, 0), (2, 3), (3, 2)]


def across(a):
    return lax.ppermute(a, "dp", ACROSS)


def sibling(a):
    return lax.ppermute(a, "dp", SIBLING)


def step(x, dy, w_gate, w_up, w_down, m_gate, m_up, m_down, v_gate, v_up, v_down):
    dp = lax.axis_index("dp")
    at = jnp.stack([dp // 2, dp % 2]).astype(jnp.int32)
    x, dy = x[0], dy[0]
    d, f = w_gate.shape[1:]

    def blocks(a):
        return a.reshape(4, a.shape[0] // 4, a.shape[1])

    dy_far = across(dy)
    a1, hid1, s1, q1, h1 = first(x, w_gate, w_up, w_down)
    h1_far = across(h1)
    a2, hid2, dgu2, d1 = second_back(h1, dy, w_gate, w_up, w_down)

    dgu1, theirs = hidden_back(at, w_down, d1, s1, q1, hid1)
    got_down = sibling(theirs)
    (theirs,) = grad_wide(at, [(blocks(a1), dgu1)], on(False, False), on(True, False), both=True)
    got_down = after(got_down, theirs)
    got_wide = sibling(theirs)
    send, keep_down1 = grad_tall(at, [(blocks(hid1), d1)], on(False, True), on(True, True), got_down)
    far_down1 = across(send)
    got_wide = after(got_wide, keep_down1)
    send, keep_wide1 = grad_wide(at, [(blocks(a1), dgu1)], on(False, True), on(True, True), got_wide)
    far_wide1 = across(send)

    h1_far = after(h1_far, keep_wide1)
    a2f, hid2f, dgu2f = second(h1_far, dy_far, w_gate, w_up, w_down)
    send, keep_wide2 = grad_wide(at, [(blocks(a2), dgu2), (blocks(a2f), dgu2f)], on(True, False), on(True, True), bn=768)
    far_wide2 = sibling(send)
    hid2f = after(hid2f, keep_wide2)
    send, keep_down2 = grad_tall(at, [(blocks(hid2), dy), (blocks(hid2f), dy_far)], on(True, False), on(True, True))
    far_down2 = sibling(send)

    most = sum_of_squares([(keep_wide1, far_wide1), (keep_down1, far_down1), (keep_wide2, far_wide2)])
    far_down2 = after(far_down2, most)
    squares = jnp.sum(most + sum_of_squares([(keep_down2, far_down2)]))
    squares = lax.psum(squares, "dp")
    factor = jnp.minimum(1.0, 0.5 * lax.rsqrt(squares / (6 * d * f) + 1e-30)).reshape(1)

    weights = {"gate": (w_gate, m_gate, v_gate), "up": (w_up, m_up, v_up), "down": (w_down, m_down, v_down)}
    grads = [
        ("gate", 1, 0, keep_wide2, far_wide2),
        ("up", 1, 1, keep_wide2, far_wide2),
        ("down", 1, 0, keep_down2[None], far_down2[None]),
        ("gate", 0, 0, keep_wide1, far_wide1),
        ("up", 0, 1, keep_wide1, far_wide1),
        ("down", 0, 0, keep_down1[None], far_down1[None]),
    ]
    placed, moments = dict.fromkeys(weights), dict.fromkeys(weights)
    for which, part in PARTS:
        name, layer, which, keep, far = grads[which]
        w, m, v = weights[name]
        own, *moments[name] = adam(at, factor, layer, which, part, keep, far, w, m, v, moments[name])
        away = across(own)
        beside = sibling(own)
        placed[name] = place(at, layer, part, (own, beside), (on(True, True), on(True, False)), w.shape, placed[name])
        away_beside = sibling(away)
        placed[name] = place(at, layer, part, (away,), (on(False, True),), w.shape, placed[name])
        placed[name] = place(at, layer, part, (away_beside,), (on(False, False),), w.shape, placed[name])
    return (*placed.values(), *(p[0] for p in moments.values()), *(p[1] for p in moments.values()))


PARTS = [(0, (0, 1)), (0, (1, 5)), (1, (0, 5)), (2, (0, 5)), (3, (0, 5)), (4, (0, 5)), (5, (0, 3)), (5, (3, 5))]


def solution(mesh):
    tokens, whole, rows = P(("rep", "dp")), P(), P(None, "dp")

    return jax.shard_map(
        step,
        mesh=mesh,
        in_specs=(tokens,) * 2 + (whole,) * 3 + (rows,) * 6,
        out_specs=(P("rep"),) * 3 + (P("rep", "dp"),) * 6,
        check_vma=False,
    )
```

```python
import functools

import jax
import jax.numpy as jnp
from jax import lax
from jax.experimental import pallas as pl
from jax.experimental.pallas import tpu as pltpu
from jax.sharding import PartitionSpec as P

BF, F32 = jnp.bfloat16, jnp.float32
NN = (((1,), (0,)), ((), ()))
NT = (((1,), (1,)), ((), ()))
CHUNK = 256
TOKENS, UNITS = 1024, 512


def dot(a, b, dims):
    return lax.dot_general(a, b, dims, preferred_element_type=F32)


def params():
    return pltpu.CompilerParams(vmem_limit_bytes=61 * 2**20)


def cost(flops, nbytes):
    return pl.CostEstimate(flops=int(flops), bytes_accessed=int(nbytes), transcendentals=0)


def out(shape, dtype=BF):
    return jax.ShapeDtypeStruct(shape, dtype)


def once(shape, index):
    return pl.BlockSpec(shape, index, pipeline_mode=pl.Buffered(1))


def call(kernel, at, grid, in_specs, out_specs, out_shape, operands, flops, nbytes, scratch=(), **kw):
    return pl.pallas_call(
        kernel,
        grid_spec=pltpu.PrefetchScalarGridSpec(
            num_scalar_prefetch=1, grid=grid, in_specs=in_specs, out_specs=out_specs, scratch_shapes=scratch
        ),
        out_shape=out_shape,
        compiler_params=params(),
        cost_estimate=cost(flops, nbytes),
        **kw,
    )(at, *operands)


def sigmoid(x):
    return 0.5 * jnp.tanh(0.5 * x) + 0.5


def chunks(n, size=CHUNK):
    return [slice(at, min(at + size, n)) for at in range(0, n, size)]


def loop(n, size, body):
    lax.fori_loop(0, n, lambda i, _: body(pl.ds(pl.multiple_of(i * size, size), size)), None)


def norm(h, a, a_out):
    def rows(r):
        wide = h[r, :].astype(F32)
        scale = lax.rsqrt(jnp.mean(wide * wide, -1, keepdims=True) + 1e-6)
        a[r, :] = (wide * scale).astype(BF)
        a_out[:, r] = a[r, :].T

    loop(a.shape[0] // CHUNK, CHUNK, rows)


def only(a, n, axis):
    return jnp.where(lax.broadcasted_iota(jnp.int32, a.shape, axis) < n, a, jnp.zeros_like(a))


def first_kernel(at, x, wg, wu, wd, m, v, a_out, hid, s_out, q_out, h_out, half, a, units, total, *, f):
    j = pl.program_id(1)
    left = f - j * UNITS
    half[...] = jnp.where(at[2] == 0, m[...], v[...])

    @pl.when(j == 0)
    def _():
        norm(x, a, a_out)
        total[...] = jnp.zeros_like(total)

    for c in chunks(UNITS):
        gate, up = dot(a[...], wg[:, c], NN), dot(a[...], wu[:, c], NN)
        sig = sigmoid(gate)
        silu = gate * sig
        units[:, c] = only((silu * up).astype(BF), left - c.start, 1)
        hid[c, :] = units[:, c].T
        s_out[:, c] = silu
        q_out[:, c] = up * (sig + silu * (1 - sig))
    for c in chunks(total.shape[1]):
        total[:, c] += dot(units[...], only(wd[:, c], left, 0), NN)

    @pl.when(j == pl.num_programs(1) - 1)
    def _():
        def rows(r):
            h_out[r, :] = x[r, :] + total[r, :].astype(BF)

        loop(x.shape[0] // CHUNK, CHUNK, rows)


def first(at, x, w_gate, w_up, w_down, m, v):
    t, d = x.shape
    f = w_gate.shape[2]
    n = pl.cdiv(f, UNITS)
    wide = pl.BlockSpec((TOKENS, UNITS), lambda i, j, at: (i, j))
    weight = pl.BlockSpec((None, d, UNITS), lambda i, j, at: (0, 0, j))
    state = pl.BlockSpec((TOKENS, d), lambda i, j, at: (i, 0))
    cols = UNITS * TOKENS // t

    def moment(rep):
        return pl.BlockSpec((None, m.shape[1], cols), lambda i, j, at: (1, 0, jnp.where(at[2] == rep, i * n + j, 0)))

    return call(
        functools.partial(first_kernel, f=f),
        at,
        (t // TOKENS, n),
        [state, weight, weight, pl.BlockSpec((None, UNITS, d), lambda i, j, at: (0, j, 0)), moment(0), moment(1)],
        [
            pl.BlockSpec((d, TOKENS), lambda i, j, at: (0, i)),
            pl.BlockSpec((UNITS, TOKENS), lambda i, j, at: (j, i)),
            wide,
            wide,
            state,
            pl.BlockSpec((m.shape[1], cols), lambda i, j, at: (0, i * n + j)),
        ],
        [out((d, t)), out((f, t)), out((t, f), F32), out((t, f), F32), out((t, d)), out(m.shape[1:], F32)],
        (x, w_gate, w_up, w_down, m, v),
        6 * t * d * f,
        190e6,
        scratch=[pltpu.VMEM((TOKENS, d), BF), pltpu.VMEM((TOKENS, UNITS), BF), pltpu.VMEM((TOKENS, d), F32)],
    )


def second_units(a, dy, wg, wu, wd, hid, dgu, left):
    for c in chunks(UNITS):
        gate, up = dot(a[...], wg[:, c], NN), dot(a[...], wu[:, c], NN)
        back = dot(dy[...], wd[c, :], NT).astype(BF).astype(F32)
        sig = sigmoid(gate)
        silu = gate * sig
        hid[c, :] = (silu * up).astype(BF).T
        dgu[0, :, c] = only((back * (up * (sig + silu * (1 - sig)))).astype(BF), left - c.start, 1)
        dgu[1, :, c] = only((back * silu).astype(BF), left - c.start, 1)


def second_kernel(at, h, dy, wg, wu, wd, a_before, dgu_before, a_out, dgu, hid, a, *, f):
    j = pl.program_id(1)

    @pl.when(j == 0)
    def _():
        norm(h, a, a_out)

    second_units(a, dy, wg, wu, wd, hid, dgu, f - j * UNITS)


def second_back_kernel(at, h, dy, wg, wu, wd, a_out, dgu, hid, d_out, a, of_gate, of_up, *, f):
    j = pl.program_id(1)
    left = f - j * UNITS

    @pl.when(j == 0)
    def _():
        norm(h, a, a_out)
        of_gate[...] = jnp.zeros_like(of_gate)
        of_up[...] = jnp.zeros_like(of_up)

    second_units(a, dy, wg, wu, wd, hid, dgu, left)
    for c in chunks(of_gate.shape[1]):
        of_gate[:, c] += dot(dgu[0], only(wg[c, :], left, 1), NT)
        of_up[:, c] += dot(dgu[1], only(wu[c, :], left, 1), NT)

    @pl.when(j == pl.num_programs(1) - 1)
    def _():
        def rows(r):
            da = (of_gate[r, :].astype(BF) + of_up[r, :].astype(BF)).astype(F32)
            wide = h[r, :].astype(F32)
            scale = lax.rsqrt(jnp.mean(wide * wide, -1, keepdims=True) + 1e-6)
            along = jnp.mean(da * wide, -1, keepdims=True) * (scale * scale * scale)
            d_out[r, :] = dy[r, :] + (da * scale - wide * along).astype(BF)

        loop(h.shape[0] // CHUNK, CHUNK, rows)


def second(at, h, dy, w_gate, w_up, w_down, before=None):
    t, d = h.shape
    f = w_gate.shape[2]
    weight = pl.BlockSpec((None, d, UNITS), lambda i, j, at: (1, 0, j))
    state = pl.BlockSpec((TOKENS, d), lambda i, j, at: (i, 0))
    far = before is not None
    which = (lambda at: 1 - at[0]) if far else (lambda at: at[0])
    in_specs = [state, state, weight, weight, pl.BlockSpec((None, UNITS, d), lambda i, j, at: (1, j, 0))]
    out_specs = [
        pl.BlockSpec((None, d, TOKENS), lambda i, j, at: (which(at), 0, i)),
        pl.BlockSpec((None, 2, TOKENS, UNITS), lambda i, j, at: (which(at), 0, i, j)),
        pl.BlockSpec((UNITS, TOKENS), lambda i, j, at: (j, i)),
    ]
    shapes = [out((2, d, t)), out((2, 2, t, f)), out((f, t))]
    scratch = [pltpu.VMEM((TOKENS, d), BF)]
    operands = [h, dy, w_gate, w_up, w_down]
    aliases = {}
    if far:
        aliases = {6: 0, 7: 1}
        in_specs += [pl.BlockSpec(memory_space=pl.ANY)] * 2
        operands += before
    else:
        out_specs.append(state)
        shapes.append(out((t, d)))
        scratch += [pltpu.VMEM((TOKENS, d), F32)] * 2
    return pl.pallas_call(
        functools.partial(second_kernel if far else second_back_kernel, f=f),
        grid_spec=pltpu.PrefetchScalarGridSpec(
            num_scalar_prefetch=1,
            grid=(t // TOKENS, pl.cdiv(f, UNITS)),
            in_specs=in_specs,
            out_specs=out_specs,
            scratch_shapes=scratch,
        ),
        out_shape=shapes,
        input_output_aliases=aliases,
        compiler_params=params(),
        cost_estimate=cost((6 if far else 10) * t * d * f, 130e6),
        name="second" if far else "second_back",
    )(at, *operands)


def on(x_same, core_same):
    def block(at):
        return 2 * (at[0] if x_same else 1 - at[0]) + (at[1] if core_same else 1 - at[1])

    return block


def hidden_back_kernel(at, w, d, s, q, one, two, dgu, theirs):
    for c in chunks(UNITS):
        back = dot(d[...], w[c, :], NT).astype(BF).astype(F32)
        dgu[1, :, c] = (back * s[:, c]).astype(BF)
        dgu[0, :, c] = (back * q[:, c]).astype(BF)
    left = jnp.concatenate([one[...], two[...]], 0)
    for which in range(2):
        theirs[which] = dot(left, dgu[which], NN).reshape(theirs.shape[1:]).astype(BF)


def hidden_back(at, w_down, d_h, s, q, a):
    t, d = d_h.shape
    f = s.shape[1]
    rows = a.shape[1]
    wide = pl.BlockSpec((t, UNITS), lambda j, at: (0, j))
    return call(
        hidden_back_kernel,
        at,
        (pl.cdiv(f, UNITS),),
        [
            pl.BlockSpec((None, UNITS, d), lambda j, at: (0, j, 0)),
            once((t, d), lambda j, at: (0, 0)),
            wide,
            wide,
            once((None, rows, t), lambda j, at: (on(False, False)(at), 0, 0)),
            once((None, rows, t), lambda j, at: (on(True, False)(at), 0, 0)),
        ],
        [pl.BlockSpec((2, t, UNITS), lambda j, at: (0, 0, j)), pl.BlockSpec((2, 2, rows, UNITS), lambda j, at: (0, 0, 0, j))],
        [out((2, t, f)), out((2, 2, rows, f))],
        (w_down, d_h, s, q, a, a),
        4 * t * d * f,
        160e6,
    )


def wide_kernel(at, one, two, right, got, send, keep):
    rows = one.shape[0]
    total = dot(jnp.concatenate([one[...], two[...]], 0), right[...], NN)
    total = total + got[...].reshape(total.shape).astype(F32)
    send[...], keep[...] = total[:rows].astype(BF), total[rows:]


def grad_wide(at, left, right, one, two, got):
    rows, t = left.shape[1:]
    f = right.shape[2]
    bn = 1536
    return call(
        wide_kernel,
        at,
        (2, pl.cdiv(f, bn)),
        [once((None, rows, t), lambda w, j, at, b=b: (b(at), 0, 0)) for b in (one, two)]
        + [pl.BlockSpec((None, t, bn), lambda w, j, at: (w, 0, j)), pl.BlockSpec((None, 2, rows, bn), lambda w, j, at: (w, 0, 0, j))],
        [pl.BlockSpec((None, rows, bn), lambda w, j, at: (w, 0, j))] * 2,
        [out((2, rows, f)), out((2, rows, f), F32)],
        (left, left, right, got),
        8 * rows * t * f,
        60e6,
    )


def whole_kernel(at, left0, left1, right0, right1, send_far, keep_far, send, keep, total):
    x, c = at[0], at[1]
    rows = send.shape[0]

    def product(r):
        return (dot(left0[r, :], right0[...], NN) + dot(left1[r, :], right1[...], NN)).reshape(-1, *total.shape[1:])

    @pl.when(pl.program_id(0) == 0)
    def _():
        total[...] = product(slice(None))
        send_far[...], keep_far[...] = total[2 * (1 - x) + 1 - c].astype(BF), total[2 * (1 - x) + c]
        send[...], keep[...] = total[2 * x + 1 - c].astype(BF), total[2 * x + c]

    @pl.when(pl.program_id(0) == 1)
    def _():
        total[:2] = product(pl.ds(pl.multiple_of(x * 2 * rows, 2 * rows), 2 * rows))
        send[...], keep[...] = total[1 - c].astype(BF), total[c]


def grad_whole(at, left, right):
    d, t = left.shape[1:]
    f = right.shape[3]
    rows, bn = d // 4, 768
    n = pl.cdiv(f, bn)
    far = pl.BlockSpec((rows, bn), lambda w, j, at: (0, jnp.where(w == 0, j, n - 1)))
    same = pl.BlockSpec((None, rows, bn), lambda w, j, at: (w, 0, j))
    return call(
        whole_kernel,
        at,
        (2, n),
        [once((None, d, t), lambda w, j, at, x=x: (x, 0, 0)) for x in range(2)]
        + [pl.BlockSpec((None, None, t, bn), lambda w, j, at, x=x: (x, w, 0, j)) for x in range(2)],
        [far, far, same, same],
        [out((rows, f)), out((rows, f), F32), out((2, rows, f)), out((2, rows, f), F32)],
        (left, left, right, right),
        6 * d * t * f,
        120e6,
        scratch=[pltpu.VMEM((4, rows, bn), F32)],
    )


def tall_kernel(at, *refs, terms, add, keeps):
    operands, rest = refs[: 2 * terms], refs[2 * terms :]
    half = pl.num_programs(0) // 2
    total = 0
    for left, right in zip(operands[::2], operands[1::2], strict=True):
        total = total + dot(left[...], right[...], NN)
    if add:
        total = total + rest[0][...].astype(F32)
    if not keeps:
        rest[-1][...] = total.astype(BF)
        return

    @pl.when(pl.program_id(0) < half)
    def _():
        rest[-2][...] = total.astype(BF)

    @pl.when(pl.program_id(0) >= half)
    def _():
        rest[-1][...] = total


def grad_tall(at, pairs, one, two, got=None, keeps=True, half=2):
    rows, t = pairs[0][0].shape[1:]
    d = pairs[0][1].shape[1]
    bm = rows // half
    in_specs, operands = [], []
    for left, right in pairs:
        in_specs += [
            pl.BlockSpec((None, bm, t), lambda j, at: (jnp.where(j < half, one(at), two(at)), j % half, 0)),
            once(right.shape, lambda j, at: (0, 0)),
        ]
        operands += [left, right]
    if got is not None:
        in_specs.append(pl.BlockSpec((None, bm, d), lambda j, at: (j // half, j % half, 0)))
        operands.append(got)
    if keeps:
        out_specs = [pl.BlockSpec((bm, d), lambda j, at: (jnp.minimum(j, half - 1), 0)), pl.BlockSpec((bm, d), lambda j, at: (jnp.maximum(j - half, 0), 0))]
        shapes = [out((rows, d)), out((rows, d), F32)]
    else:
        out_specs = [pl.BlockSpec((None, bm, d), lambda j, at: (j // half, j % half, 0))]
        shapes = [out((2, rows, d))]
    return call(
        functools.partial(tall_kernel, terms=len(pairs), add=got is not None, keeps=keeps),
        at,
        (2 * half,),
        in_specs,
        out_specs,
        shapes,
        operands,
        4 * rows * t * d * len(pairs),
        60e6,
    )


def squares_of(keep, far):
    g = (keep[...] + far[...].astype(F32)).astype(BF).astype(F32)
    g = jnp.sum((g * g).reshape(-1, 8, g.shape[-1]), 0)
    return sum(g[:, c] for c in chunks(g.shape[1], 128))


def squares_kernel(*refs):
    o = refs[-1]

    @pl.when(pl.program_id(0) == 0)
    def _():
        o[...] = jnp.zeros_like(o)

    o[...] += sum(squares_of(keep, far) for keep, far in zip(refs[:-1:2], refs[1:-1:2], strict=True))


def sum_of_squares(pairs, n):
    specs = []
    for a, _ in pairs:
        br = a.shape[-2] // n
        if a.ndim == 2:
            spec = pl.BlockSpec((br, a.shape[1]), lambda i: (i, 0))
        else:
            spec = pl.BlockSpec((a.shape[0], br, a.shape[2]), lambda i: (0, i, 0))
        specs += [spec, spec]
    return pl.pallas_call(
        squares_kernel,
        grid=(n,),
        in_specs=specs,
        out_specs=pl.BlockSpec((8, 128), lambda i: (0, 0)),
        out_shape=out((8, 128), F32),
        compiler_params=params(),
        cost_estimate=cost(1e9, 4e6 * len(specs)),
        name="squares",
    )(*[a for pair in pairs for a in pair])


UNITS_OF_ROWS = 5


def updated(g, w, m, v):
    m = 0.9 * m + 0.1 * g
    v = 0.95 * v + 0.05 * g * g
    wide = w.astype(F32)
    return (wide - 0.02 * (m * lax.rsqrt(v + 1e-8) + 0.1 * wide)).astype(BF), m, v


def gradient(factor, keep, far):
    return (keep[...] + far[...].astype(F32)).astype(BF).astype(F32) * factor[0]


def adam_kernel(at, factor, keep, far, w, m, v, *rest):
    w_out, m_out, v_out, w_new = rest[-4:]
    w_out[...], m_out[...], v_out[...] = updated(gradient(factor, keep, far), w[...], m[...], v[...])
    w_new[...] = w_out[...]


def adam(at, factor, layer, which, part, keep, far, w, m, v, before):
    rows, cols = keep.shape[1:]
    br = rows // UNITS_OF_ROWS
    low, high = part
    own = pl.BlockSpec((None, br, cols), lambda i, at: (layer, low + i, 0))
    grad = pl.BlockSpec((None, br, cols), lambda i, at: (which, low + i, 0))
    there = pl.BlockSpec((None, br, cols), lambda i, at: (layer, (2 * at[0] + at[1]) * UNITS_OF_ROWS + low + i, 0))
    return call(
        adam_kernel,
        at,
        (high - low,),
        [pl.BlockSpec(memory_space=pltpu.SMEM), grad, grad, there, own, own] + [pl.BlockSpec(memory_space=pl.ANY)] * len(before),
        [pl.BlockSpec((br, cols), lambda i, at: (i, 0)), own, own, there],
        [out((br * (high - low), cols)), out(m.shape, F32), out(v.shape, F32), out(w.shape)],
        [factor, keep, far, w, m, v, *before],
        1e9,
        6e6 * (high - low),
        input_output_aliases={7: 1, 8: 2, 9: 3} if before else {},
    )


def adam_far_kernel(at, factor, keep, far, w, crossed, handed, before, w_out, w_new):
    m, v = jnp.where(at[2] == 0, crossed[...], handed[...]), jnp.where(at[2] == 0, handed[...], crossed[...])
    w_out[...], _, _ = updated(gradient(factor, keep, far), w[...], m, v)
    w_new[...] = w_out[...]


def adam_far(at, factor, layer, keep, far, w, crossed, handed, before):
    rows, cols = keep.shape
    br = rows // UNITS_OF_ROWS
    flat = pl.BlockSpec((br, cols), lambda i, at: (i, 0))
    there = pl.BlockSpec((None, br, cols), lambda i, at: (layer, (2 * (1 - at[0]) + at[1]) * UNITS_OF_ROWS + i, 0))
    return call(
        adam_far_kernel,
        at,
        (UNITS_OF_ROWS,),
        [pl.BlockSpec(memory_space=pltpu.SMEM), flat, flat, there, flat, flat, pl.BlockSpec(memory_space=pl.ANY)],
        [flat, there],
        [out((rows, cols)), out(w.shape)],
        [factor, keep, far, w, crossed, handed, before],
        1e9,
        30e6,
        input_output_aliases={7: 1},
    )


def place_kernel(at, *refs, count):
    for n in range(count):
        pl.when(pl.program_id(0) == n)(functools.partial(lambda n: refs[-1].__setitem__(..., refs[n][...]), n))


def place(at, layer, part, blocks, wheres, before):
    low, high = part
    k = high - low
    cols = blocks[0].shape[1]
    br = blocks[0].shape[0] // k

    def spec(n):
        return pl.BlockSpec((br, cols), lambda i, j, at: (jnp.where(i < n, 0, jnp.where(i > n, k - 1, j)), 0))

    def where(i, j, at):
        b = wheres[0](at)
        for n, w in enumerate(wheres[1:], 1):
            b = jnp.where(i == n, w(at), b)
        return layer, b * UNITS_OF_ROWS + low + j, 0

    return call(
        functools.partial(place_kernel, count=len(blocks)),
        at,
        (len(blocks), k),
        [spec(n) for n in range(len(blocks))] + [pl.BlockSpec(memory_space=pl.ANY)],
        pl.BlockSpec((None, br, cols), where),
        out(before.shape),
        [*blocks, before],
        1e9,
        1.2e6 * k * len(blocks),
        input_output_aliases={1 + len(blocks): 0},
    )


def after(value, *others):
    return lax.optimization_barrier((value, *others))[0]


ACROSS = [(0, 2), (2, 0), (1, 3), (3, 1)]
SIBLING = [(0, 1), (1, 0), (2, 3), (3, 2)]


def across(a):
    return lax.ppermute(a, "dp", ACROSS)


def sibling(a):
    return lax.ppermute(a, "dp", SIBLING)


def step(x, dy, w_gate, w_up, w_down, m_gate, m_up, m_down, v_gate, v_up, v_down):
    dp = lax.axis_index("dp")
    at = jnp.stack([dp // 2, dp % 2, lax.axis_index("rep")]).astype(jnp.int32)
    x, dy = x[0], dy[0]
    d, f = w_gate.shape[1:]

    def blocks(a):
        return a.reshape(4, a.shape[0] // 4, a.shape[1])

    dy_far = across(dy)
    a1, hid1, s1, q1, h1, half = first(at, x, w_gate, w_up, w_down, m_gate, v_gate)
    h1_far = across(h1)
    crossed = across(half)
    handed = lax.ppermute(crossed, "rep", [(0, 1), (1, 0)])
    a2, dgu2, hid2, d1 = second(at, h1, dy, w_gate, w_up, w_down)

    dgu1, theirs = hidden_back(at, w_down, d1, s1, q1, blocks(a1))
    got_wide = sibling(theirs)
    pairs = [(blocks(hid1), after(d1, theirs))]
    (theirs,) = grad_tall(at, pairs, on(False, False), on(True, False), keeps=False)
    got_down = sibling(theirs)
    got_wide = after(got_wide, theirs)
    send, keep_wide1 = grad_wide(at, blocks(a1), dgu1, on(False, True), on(True, True), got_wide)
    far_wide1 = across(send)
    got_down = after(got_down, keep_wide1)
    send, keep_down1 = grad_tall(at, pairs, on(False, True), on(True, True), got_down)
    far_down1 = across(send)

    h1_far = after(h1_far, keep_down1)
    a2, dgu2, hid2f = second(at, h1_far, dy_far, w_gate, w_up, w_down, [a2, dgu2])
    send, keep_other, send_wide, keep_wide2 = grad_whole(at, a2, dgu2)
    far_other, far_wide2 = sibling(send), sibling(send_wide)
    pairs = [(blocks(hid2), dy), (blocks(after(hid2f, keep_wide2)), dy_far)]
    send, keep_down2 = grad_tall(at, pairs, on(True, False), on(True, True))
    far_down2 = sibling(send)

    most = sum_of_squares([(keep_wide2, far_wide2), (keep_down1, far_down1), (keep_wide1, far_wide1)], 10)
    far_down2 = after(far_down2, most)
    squares = jnp.sum(most + sum_of_squares([(keep_down2, far_down2)], 5))
    squares = lax.psum(squares, "dp")
    factor = jnp.minimum(1.0, 0.5 * lax.rsqrt(squares / (6 * d * f) + 1e-30)).reshape(1)

    weights = {"gate": (w_gate, m_gate, v_gate), "up": (w_up, m_up, v_up), "down": (w_down, m_down, v_down)}
    grads = {
        "gate1": (1, 0, keep_wide2, far_wide2),
        "up1": (1, 1, keep_wide2, far_wide2),
        "down1": (1, 0, keep_down2[None], far_down2[None]),
        "gate0": (0, 0, keep_wide1, far_wide1),
        "up0": (0, 1, keep_wide1, far_wide1),
        "down0": (0, 0, keep_down1[None], far_down1[None]),
    }
    new = dict.fromkeys(weights, ())

    def update(which, part):
        name = which[:-1]
        own, *new[name] = adam(at, factor, *grads[which][:2], part, *grads[which][2:], *weights[name], new[name])
        return own

    def put(which, part, *blocks):
        name = which[:-1]
        *moments, w = new[name]
        where, arrays = zip(*blocks, strict=True)
        new[name] = [*moments, place(at, grads[which][0], part, arrays, where, w)]

    whole = (0, UNITS_OF_ROWS)
    own = update("gate1", whole)
    *moments, w = new["gate"]
    away, w = adam_far(at, factor, 1, keep_other, far_other, w_gate, crossed, handed, w)
    new["gate"] = [*moments, w]
    put("gate1", whole, (on(True, False), sibling(own)), (on(False, False), sibling(away)))

    parts = []
    for n, (which, part) in enumerate(PARTS):
        own = update(which, part)
        parts.append((across(own), sibling(own)))
        if n in LATER:
            continue
        for n, (away, beside) in enumerate(parts):
            if away is not None:
                which, part = PARTS[n]
                put(which, part, (on(True, False), beside))
                put(which, part, (on(False, True), away))
                put(which, part, (on(False, False), sibling(away)))
                parts[n] = None, None
    return tuple(new[name][i] for i in (2, 0, 1) for name in weights)


PARTS = [("up1", (0, 1)), ("up1", (1, 5)), ("down1", (0, 5)), ("gate0", (0, 5)), ("up0", (0, 5)), ("down0", (0, 3)), ("down0", (3, 5))]
LATER = (0, 5)


def solution(mesh):
    tokens, whole, rows = P(("rep", "dp")), P(), P(None, "dp")

    return jax.shard_map(
        step,
        mesh=mesh,
        in_specs=(tokens,) * 2 + (whole,) * 3 + (rows,) * 6,
        out_specs=(P("rep"),) * 3 + (P("rep", "dp"),) * 6,
        check_vma=False,
    )
```

```python
import functools

import jax
import jax.numpy as jnp
from jax import lax
from jax.experimental import pallas as pl
from jax.experimental.pallas import tpu as pltpu
from jax.sharding import PartitionSpec as P

BF, F32 = jnp.bfloat16, jnp.float32
NN = (((1,), (0,)), ((), ()))
NT = (((1,), (1,)), ((), ()))
CHUNK = 256
TOKENS, UNITS = 1024, 512


def dot(a, b, dims):
    return lax.dot_general(a, b, dims, preferred_element_type=F32)


def params():
    return pltpu.CompilerParams(vmem_limit_bytes=61 * 2**20)


def cost(flops, nbytes):
    return pl.CostEstimate(flops=int(flops), bytes_accessed=int(nbytes), transcendentals=0)


def out(shape, dtype=BF):
    return jax.ShapeDtypeStruct(shape, dtype)


def once(shape, index):
    return pl.BlockSpec(shape, index, pipeline_mode=pl.Buffered(1))


def call(kernel, at, grid, in_specs, out_specs, out_shape, operands, flops, nbytes, scratch=(), **kw):
    return pl.pallas_call(
        kernel,
        grid_spec=pltpu.PrefetchScalarGridSpec(
            num_scalar_prefetch=1, grid=grid, in_specs=in_specs, out_specs=out_specs, scratch_shapes=scratch
        ),
        out_shape=out_shape,
        compiler_params=params(),
        cost_estimate=cost(flops, nbytes),
        **kw,
    )(at, *operands)


def sigmoid(x):
    return 0.5 * jnp.tanh(0.5 * x) + 0.5


def chunks(n, size=CHUNK):
    return [slice(at, min(at + size, n)) for at in range(0, n, size)]


def loop(n, size, body):
    lax.fori_loop(0, n, lambda i, _: body(pl.ds(pl.multiple_of(i * size, size), size)), None)


def norm(h, a, a_out):
    def rows(r):
        wide = h[r, :].astype(F32)
        scale = lax.rsqrt(jnp.mean(wide * wide, -1, keepdims=True) + 1e-6)
        a[r, :] = (wide * scale).astype(BF)
        a_out[:, r] = a[r, :].T

    loop(a.shape[0] // CHUNK, CHUNK, rows)


def only(a, n, axis):
    return jnp.where(lax.broadcasted_iota(jnp.int32, a.shape, axis) < n, a, jnp.zeros_like(a))


def first_kernel(at, x, wg, wu, wd, mg, vg, mu, vu, a_out, hid, s_out, q_out, h_out, half_gate, half_up, a, units, total, *, f):
    j = pl.program_id(1)
    left = f - j * UNITS
    half_gate[...] = jnp.where(at[2] == 0, mg[...], vg[...])
    half_up[...] = jnp.where(at[2] == 0, mu[...], vu[...])

    @pl.when(j == 0)
    def _():
        norm(x, a, a_out)
        total[...] = jnp.zeros_like(total)

    for c in chunks(UNITS):
        gate, up = dot(a[...], wg[:, c], NN), dot(a[...], wu[:, c], NN)
        sig = sigmoid(gate)
        silu = gate * sig
        units[:, c] = only((silu * up).astype(BF), left - c.start, 1)
        hid[c, :] = units[:, c].T
        s_out[:, c] = silu
        q_out[:, c] = up * (sig + silu * (1 - sig))
    for c in chunks(total.shape[1]):
        total[:, c] += dot(units[...], only(wd[:, c], left, 0), NN)

    @pl.when(j == pl.num_programs(1) - 1)
    def _():
        def rows(r):
            h_out[r, :] = x[r, :] + total[r, :].astype(BF)

        loop(x.shape[0] // CHUNK, CHUNK, rows)


def first(at, x, w_gate, w_up, w_down, moments):
    m = moments[0]
    t, d = x.shape
    f = w_gate.shape[2]
    n = pl.cdiv(f, UNITS)
    wide = pl.BlockSpec((TOKENS, UNITS), lambda i, j, at: (i, j))
    weight = pl.BlockSpec((None, d, UNITS), lambda i, j, at: (0, 0, j))
    state = pl.BlockSpec((TOKENS, d), lambda i, j, at: (i, 0))
    cols = UNITS * TOKENS // t

    def moment(rep):
        return pl.BlockSpec((None, m.shape[1], cols), lambda i, j, at: (1, 0, jnp.where(at[2] == rep, i * n + j, 0)))

    return call(
        functools.partial(first_kernel, f=f),
        at,
        (t // TOKENS, n),
        [state, weight, weight, pl.BlockSpec((None, UNITS, d), lambda i, j, at: (0, j, 0)), *[moment(0), moment(1)] * 2],
        [
            pl.BlockSpec((d, TOKENS), lambda i, j, at: (0, i)),
            pl.BlockSpec((UNITS, TOKENS), lambda i, j, at: (j, i)),
            wide,
            wide,
            state,
        ]
        + [pl.BlockSpec((m.shape[1], cols), lambda i, j, at: (0, i * n + j))] * 2,
        [out((d, t)), out((f, t)), out((t, f), F32), out((t, f), F32), out((t, d))] + [out(m.shape[1:], F32)] * 2,
        (x, w_gate, w_up, w_down, *moments),
        6 * t * d * f,
        190e6,
        scratch=[pltpu.VMEM((TOKENS, d), BF), pltpu.VMEM((TOKENS, UNITS), BF), pltpu.VMEM((TOKENS, d), F32)],
    )


def second_units(a, dy, wg, wu, wd, hid, dgu, left):
    for c in chunks(UNITS):
        gate, up = dot(a[...], wg[:, c], NN), dot(a[...], wu[:, c], NN)
        back = dot(dy[...], wd[c, :], NT).astype(BF).astype(F32)
        sig = sigmoid(gate)
        silu = gate * sig
        hid[c, :] = (silu * up).astype(BF).T
        dgu[0, :, c] = only((back * (up * (sig + silu * (1 - sig)))).astype(BF), left - c.start, 1)
        dgu[1, :, c] = only((back * silu).astype(BF), left - c.start, 1)


def second_kernel(at, h, dy, wg, wu, wd, a_before, dgu_before, a_out, dgu, hid, a, *, f):
    j = pl.program_id(1)

    @pl.when(j == 0)
    def _():
        norm(h, a, a_out)

    second_units(a, dy, wg, wu, wd, hid, dgu, f - j * UNITS)


def second_back_kernel(at, h, dy, wg, wu, wd, a_out, dgu, hid, d_out, a, of_gate, of_up, *, f):
    j = pl.program_id(1)
    left = f - j * UNITS

    @pl.when(j == 0)
    def _():
        norm(h, a, a_out)
        of_gate[...] = jnp.zeros_like(of_gate)
        of_up[...] = jnp.zeros_like(of_up)

    second_units(a, dy, wg, wu, wd, hid, dgu, left)
    for c in chunks(of_gate.shape[1]):
        of_gate[:, c] += dot(dgu[0], only(wg[c, :], left, 1), NT)
        of_up[:, c] += dot(dgu[1], only(wu[c, :], left, 1), NT)

    @pl.when(j == pl.num_programs(1) - 1)
    def _():
        def rows(r):
            da = (of_gate[r, :].astype(BF) + of_up[r, :].astype(BF)).astype(F32)
            wide = h[r, :].astype(F32)
            scale = lax.rsqrt(jnp.mean(wide * wide, -1, keepdims=True) + 1e-6)
            along = jnp.mean(da * wide, -1, keepdims=True) * (scale * scale * scale)
            d_out[r, :] = dy[r, :] + (da * scale - wide * along).astype(BF)

        loop(h.shape[0] // CHUNK, CHUNK, rows)


def second(at, h, dy, w_gate, w_up, w_down, before=None):
    t, d = h.shape
    f = w_gate.shape[2]
    far = before is not None
    bt = TOKENS // 2 if far else TOKENS
    weight = pl.BlockSpec((None, d, UNITS), lambda i, j, at: (1, 0, j))
    state = pl.BlockSpec((bt, d), lambda i, j, at: (i, 0))
    which = (lambda at: 1 - at[0]) if far else (lambda at: at[0])
    in_specs = [state, state, weight, weight, pl.BlockSpec((None, UNITS, d), lambda i, j, at: (1, j, 0))]
    out_specs = [
        pl.BlockSpec((None, d, bt), lambda i, j, at: (which(at), 0, i)),
        pl.BlockSpec((None, 2, bt, UNITS), lambda i, j, at: (which(at), 0, i, j)),
        pl.BlockSpec((UNITS, bt), lambda i, j, at: (j, i)),
    ]
    shapes = [out((2, d, t)), out((2, 2, t, f)), out((f, t))]
    scratch = [pltpu.VMEM((bt, d), BF)]
    operands = [h, dy, w_gate, w_up, w_down]
    aliases = {}
    if far:
        aliases = {6: 0, 7: 1}
        in_specs += [pl.BlockSpec(memory_space=pl.ANY)] * 2
        operands += before
    else:
        out_specs.append(state)
        shapes.append(out((t, d)))
        scratch += [pltpu.VMEM((bt, d), F32)] * 2
    return pl.pallas_call(
        functools.partial(second_kernel if far else second_back_kernel, f=f),
        grid_spec=pltpu.PrefetchScalarGridSpec(
            num_scalar_prefetch=1,
            grid=(t // bt, pl.cdiv(f, UNITS)),
            in_specs=in_specs,
            out_specs=out_specs,
            scratch_shapes=scratch,
        ),
        out_shape=shapes,
        input_output_aliases=aliases,
        compiler_params=params(),
        cost_estimate=cost((6 if far else 10) * t * d * f, 130e6),
        name="second" if far else "second_back",
    )(at, *operands)


def on(x_same, core_same):
    def block(at):
        return 2 * (at[0] if x_same else 1 - at[0]) + (at[1] if core_same else 1 - at[1])

    return block


def hidden_back_kernel(at, w, d, s, q, one, two, dgu, theirs):
    for c in chunks(UNITS):
        back = dot(d[...], w[c, :], NT).astype(BF).astype(F32)
        dgu[1, :, c] = (back * s[:, c]).astype(BF)
        dgu[0, :, c] = (back * q[:, c]).astype(BF)
    left = jnp.concatenate([one[...], two[...]], 0)
    for which in range(2):
        theirs[which] = dot(left, dgu[which], NN).reshape(theirs.shape[1:]).astype(BF)


def hidden_back(at, w_down, d_h, s, q, a):
    t, d = d_h.shape
    f = s.shape[1]
    rows = a.shape[1]
    wide = pl.BlockSpec((t, UNITS), lambda j, at: (0, j))
    return call(
        hidden_back_kernel,
        at,
        (pl.cdiv(f, UNITS),),
        [
            pl.BlockSpec((None, UNITS, d), lambda j, at: (0, j, 0)),
            once((t, d), lambda j, at: (0, 0)),
            wide,
            wide,
            once((None, rows, t), lambda j, at: (on(False, False)(at), 0, 0)),
            once((None, rows, t), lambda j, at: (on(True, False)(at), 0, 0)),
        ],
        [pl.BlockSpec((2, t, UNITS), lambda j, at: (0, 0, j)), pl.BlockSpec((2, 2, rows, UNITS), lambda j, at: (0, 0, 0, j))],
        [out((2, t, f)), out((2, 2, rows, f))],
        (w_down, d_h, s, q, a, a),
        4 * t * d * f,
        160e6,
    )


def wide_kernel(at, one, two, right, got, send, keep):
    rows = one.shape[0]
    total = dot(jnp.concatenate([one[...], two[...]], 0), right[...], NN)
    total = total + got[...].reshape(total.shape).astype(F32)
    send[...], keep[...] = total[:rows].astype(BF), total[rows:]


def grad_wide(at, left, right, one, two, got):
    rows, t = left.shape[1:]
    f = right.shape[2]
    bn = 768
    return call(
        wide_kernel,
        at,
        (2, pl.cdiv(f, bn)),
        [once((None, rows, t), lambda w, j, at, b=b: (b(at), 0, 0)) for b in (one, two)]
        + [pl.BlockSpec((None, t, bn), lambda w, j, at: (w, 0, j)), pl.BlockSpec((None, 2, rows, bn), lambda w, j, at: (w, 0, 0, j))],
        [pl.BlockSpec((None, rows, bn), lambda w, j, at: (w, 0, j))] * 2,
        [out((2, rows, f)), out((2, rows, f), F32)],
        (left, left, right, got),
        8 * rows * t * f,
        60e6,
    )


def whole_kernel(at, left0, left1, right0, right1, send, keep, total):
    total[...] = (dot(left0[...], right0[...], NN) + dot(left1[...], right1[...], NN)).reshape(total.shape)
    send[...], keep[...] = total[1 - at[1]].astype(BF), total[at[1]]


def grad_whole(at, left, right):
    d, t = left.shape[1:]
    f = right.shape[3]
    rows, bn = d // 4, 768
    same = pl.BlockSpec((None, rows, bn), lambda w, j, at: (w, 0, j))

    def half(w, at):
        return jnp.where(w < 2, at[0], 1 - at[0])

    return call(
        whole_kernel,
        at,
        (4, pl.cdiv(f, bn)),
        [pl.BlockSpec((None, 2 * rows, t), lambda w, j, at, x=x: (x, half(w, at), 0)) for x in range(2)]
        + [pl.BlockSpec((None, None, t, bn), lambda w, j, at, x=x: (x, w % 2, 0, j)) for x in range(2)],
        [same, same],
        [out((4, rows, f)), out((4, rows, f), F32)],
        (left, left, right, right),
        8 * d * t * f,
        120e6,
        scratch=[pltpu.VMEM((2, rows, bn), F32)],
    )


def tall_kernel(at, *refs, terms, add, keeps):
    operands, rest = refs[: 2 * terms], refs[2 * terms :]
    half = pl.num_programs(0) // 2
    total = 0
    for left, right in zip(operands[::2], operands[1::2], strict=True):
        total = total + dot(left[...], right[...], NN)
    if add:
        total = total + rest[0][...].astype(F32)
    if not keeps:
        rest[-1][...] = total.astype(BF)
        return

    @pl.when(pl.program_id(0) < half)
    def _():
        rest[-2][...] = total.astype(BF)

    @pl.when(pl.program_id(0) >= half)
    def _():
        rest[-1][...] = total


def grad_tall(at, pairs, one, two, got=None, keeps=True, half=4):
    rows, t = pairs[0][0].shape[1:]
    d = pairs[0][1].shape[1]
    bm = rows // half
    in_specs, operands = [], []
    for left, right in pairs:
        in_specs += [
            pl.BlockSpec((None, bm, t), lambda j, at: (jnp.where(j < half, one(at), two(at)), j % half, 0)),
            once(right.shape, lambda j, at: (0, 0)),
        ]
        operands += [left, right]
    if got is not None:
        in_specs.append(pl.BlockSpec((None, bm, d), lambda j, at: (j // half, j % half, 0)))
        operands.append(got)
    if keeps:
        out_specs = [pl.BlockSpec((bm, d), lambda j, at: (jnp.minimum(j, half - 1), 0)), pl.BlockSpec((bm, d), lambda j, at: (jnp.maximum(j - half, 0), 0))]
        shapes = [out((rows, d)), out((rows, d), F32)]
    else:
        out_specs = [pl.BlockSpec((None, bm, d), lambda j, at: (j // half, j % half, 0))]
        shapes = [out((2, rows, d))]
    return call(
        functools.partial(tall_kernel, terms=len(pairs), add=got is not None, keeps=keeps),
        at,
        (2 * half,),
        in_specs,
        out_specs,
        shapes,
        operands,
        4 * rows * t * d * len(pairs),
        60e6,
    )


def squares_kernel(keep, far, o, keep_in, far_in, sems, *, n):
    rows = keep_in.shape[1] // n

    def copies(i):
        r = pl.ds(i * rows, rows)
        which = pl.ds(0, keep_in.shape[0])
        return (
            pltpu.make_async_copy(keep.at[which, r], keep_in.at[:, r], sems.at[0, i]),
            pltpu.make_async_copy(far.at[which, r], far_in.at[:, r], sems.at[1, i]),
        )

    for i in range(n):
        for copy in copies(i):
            copy.start()
    o[...] = jnp.zeros_like(o)
    for i in range(n):
        for copy in copies(i):
            copy.wait()

        def add(k, _, start=i * rows):
            which, k = k // (rows // 16), k % (rows // 16)
            r = pl.ds(pl.multiple_of(start + k * 16, 16), 16)
            g = (keep_in[which, r, :] + far_in[which, r, :].astype(F32)).astype(BF).astype(F32)
            g = jnp.sum((g * g).reshape(-1, 8, g.shape[-1]), 0)
            o[...] += sum(g[:, c] for c in chunks(g.shape[1], 128))

        lax.fori_loop(0, keep_in.shape[0] * (rows // 16), add, None)


def sum_of_squares(keep, far, first):
    n = 5
    shape = (first, *keep.shape[1:])
    return pl.pallas_call(
        functools.partial(squares_kernel, n=n),
        in_specs=[pl.BlockSpec(memory_space=pl.ANY)] * 2,
        out_specs=pl.BlockSpec(memory_space=pltpu.VMEM),
        out_shape=out((8, 128), F32),
        scratch_shapes=[pltpu.VMEM(shape, F32), pltpu.VMEM(shape, BF), pltpu.SemaphoreType.DMA((2, n))],
        compiler_params=params(),
        cost_estimate=cost(1e9, 8e6),
        name="squares",
    )(keep, far)


def updated(g, w, m, v):
    m = 0.9 * m + 0.1 * g
    v = 0.95 * v + 0.05 * g * g
    wide = w.astype(F32)
    return (wide - 0.02 * (m * lax.rsqrt(v + 1e-8) + 0.1 * wide)).astype(BF), m, v


def gradient(factor, keep, far, r):
    return (keep[r, :] + far[r, :].astype(F32)).astype(BF).astype(F32) * factor[0]


def adam_kernel(at, factor, keep, far, w, m, v, *rest):
    w_out, m_out, v_out, w_new = rest[-4:]

    def rows(r):
        w_out[r, :], m_out[r, :], v_out[r, :] = updated(gradient(factor, keep, far, r), w[r, :], m[r, :], v[r, :])
        w_new[r, :] = w_out[r, :]

    loop(w.shape[0] // 16, 16, rows)


def adam(at, factor, layer, which, part, keep, far, w, m, v, before):
    rows, cols = keep.shape[1:]
    low, high, n = part
    br = rows // n
    own = pl.BlockSpec((None, br, cols), lambda i, at: (layer, low + i, 0))
    grad = pl.BlockSpec((None, br, cols), lambda i, at: (which, low + i, 0))
    there = pl.BlockSpec((None, br, cols), lambda i, at: (layer, (2 * at[0] + at[1]) * n + low + i, 0))
    return call(
        adam_kernel,
        at,
        (high - low,),
        [pl.BlockSpec(memory_space=pltpu.SMEM), grad, grad, there, own, own] + [pl.BlockSpec(memory_space=pl.ANY)] * len(before),
        [pl.BlockSpec((br, cols), lambda i, at: (i, 0)), own, own, there],
        [out((br * (high - low), cols)), out(m.shape, F32), out(v.shape, F32), out(w.shape)],
        [factor, keep, far, w, m, v, *before],
        1e9,
        6e6 * (high - low),
        input_output_aliases={7: 1, 8: 2, 9: 3} if before else {},
    )


def adam_far_kernel(at, factor, keep, far, w, crossed, handed, before, w_out, w_new):
    def rows(r):
        m, v = jnp.where(at[2] == 0, crossed[r, :], handed[r, :]), jnp.where(at[2] == 0, handed[r, :], crossed[r, :])
        w_out[r, :], _, _ = updated(gradient(factor, keep, far, r), w[r, :], m, v)
        w_new[r, :] = w_out[r, :]

    loop(w.shape[0] // 16, 16, rows)


def adam_far(at, factor, layer, which, keep, far, w, crossed, handed, before):
    rows, cols = keep.shape[1:]
    n = 2
    br = rows // n
    grad = pl.BlockSpec((None, br, cols), lambda i, at: (which, i, 0))
    flat = pl.BlockSpec((br, cols), lambda i, at: (i, 0))
    there = pl.BlockSpec((None, br, cols), lambda i, at: (layer, (2 * (1 - at[0]) + at[1]) * n + i, 0))
    return call(
        adam_far_kernel,
        at,
        (n,),
        [pl.BlockSpec(memory_space=pltpu.SMEM), grad, grad, there, flat, flat, pl.BlockSpec(memory_space=pl.ANY)],
        [flat, there],
        [out((rows, cols)), out(w.shape)],
        [factor, keep, far, w, crossed, handed, before],
        1e9,
        30e6,
        input_output_aliases={7: 1},
    )


def place_kernel(at, *refs, count):
    for n in range(count):
        pl.when(pl.program_id(0) == n)(functools.partial(lambda n: refs[-1].__setitem__(..., refs[n][...]), n))


def place(at, layer, part, blocks, wheres, before):
    low, high, n = part
    k = high - low
    cols = blocks[0].shape[1]
    br = blocks[0].shape[0] // k

    def spec(n):
        return pl.BlockSpec((br, cols), lambda i, j, at: (jnp.where(i < n, 0, jnp.where(i > n, k - 1, j)), 0))

    def where(i, j, at):
        b = wheres[0](at)
        for k, w in enumerate(wheres[1:], 1):
            b = jnp.where(i == k, w(at), b)
        return layer, b * n + low + j, 0

    return call(
        functools.partial(place_kernel, count=len(blocks)),
        at,
        (len(blocks), k),
        [spec(n) for n in range(len(blocks))] + [pl.BlockSpec(memory_space=pl.ANY)],
        pl.BlockSpec((None, br, cols), where),
        out(before.shape),
        [*blocks, before],
        1e9,
        1.2e6 * k * len(blocks),
        input_output_aliases={1 + len(blocks): 0},
    )


def after(value, *others):
    return lax.optimization_barrier((value, *others))[0]


ACROSS = [(0, 2), (2, 0), (1, 3), (3, 1)]
SIBLING = [(0, 1), (1, 0), (2, 3), (3, 2)]


def across(a):
    return lax.ppermute(a, "dp", ACROSS)


def sibling(a):
    return lax.ppermute(a, "dp", SIBLING)


def step(x, dy, w_gate, w_up, w_down, m_gate, m_up, m_down, v_gate, v_up, v_down):
    dp = lax.axis_index("dp")
    at = jnp.stack([dp // 2, dp % 2, lax.axis_index("rep")]).astype(jnp.int32)
    x, dy = x[0], dy[0]
    d, f = w_gate.shape[1:]

    def blocks(a):
        return a.reshape(4, a.shape[0] // 4, a.shape[1])

    dy_far = across(dy)
    moments = m_gate, v_gate, m_up, v_up
    a1, hid1, s1, q1, h1, half_gate, half_up = first(at, x, w_gate, w_up, w_down, moments)
    h1_far = across(h1)

    def brought(half):
        crossed = across(half)
        return crossed, lax.ppermute(crossed, "rep", [(0, 1), (1, 0)])

    far_moments = {"gate": brought(half_gate), "up": brought(half_up)}
    a2, dgu2, hid2, d1 = second(at, h1, dy, w_gate, w_up, w_down)

    dgu1, theirs = hidden_back(at, w_down, d1, s1, q1, blocks(a1))
    got_wide = sibling(theirs)
    pairs = [(blocks(hid1), after(d1, theirs))]
    (theirs,) = grad_tall(at, pairs, on(False, False), on(True, False), keeps=False)
    got_down = sibling(theirs)
    got_wide = after(got_wide, theirs)
    send, keep_wide1 = grad_wide(at, blocks(a1), dgu1, on(False, True), on(True, True), got_wide)
    far_wide1 = across(send)
    got_down = after(got_down, keep_wide1)
    send, keep_down1 = grad_tall(at, pairs, on(False, True), on(True, True), got_down, half=7)
    far_down1 = across(send)

    h1_far = after(h1_far, keep_down1)
    a2, dgu2, hid2f = second(at, h1_far, dy_far, w_gate, w_up, w_down, [a2, dgu2])
    send, keep_wide2 = grad_whole(at, a2, dgu2)
    far_wide2 = sibling(send)
    pairs = [(blocks(hid2), dy), (blocks(after(hid2f, keep_wide2)), dy_far)]
    send, keep_down2 = grad_tall(at, pairs, on(True, False), on(True, True), half=7)
    far_down2 = sibling(send)
    keep_down1, far_down1, keep_down2, far_down2 = (a[None] for a in (keep_down1, far_down1, keep_down2, far_down2))
    sums = [sum_of_squares(keep_wide1, far_wide1, 2), sum_of_squares(keep_down1, far_down1, 1)]
    sums.append(sum_of_squares(keep_wide2, after(far_wide2, *sums), 2))
    far_down2 = after(far_down2, *sums)
    squares = jnp.sum(sum(sums) + sum_of_squares(keep_down2, far_down2, 1))
    squares = lax.psum(squares, "dp")
    factor = jnp.minimum(1.0, 0.5 * lax.rsqrt(squares / (6 * d * f) + 1e-30)).reshape(1)

    weights = {"gate": (w_gate, m_gate, v_gate), "up": (w_up, m_up, v_up), "down": (w_down, m_down, v_down)}
    grads = {
        "gate1": (1, 0, keep_wide2, far_wide2),
        "up1": (1, 1, keep_wide2, far_wide2),
        "down1": (1, 0, keep_down2, far_down2),
        "gate0": (0, 0, keep_wide1, far_wide1),
        "up0": (0, 1, keep_wide1, far_wide1),
        "down0": (0, 0, keep_down1, far_down1),
    }
    new = dict.fromkeys(weights, ())

    def update(which, part):
        name = which[:-1]
        own, *new[name] = adam(at, factor, *grads[which][:2], part, *grads[which][2:], *weights[name], new[name])
        return own

    def put(which, part, *blocks):
        name = which[:-1]
        *moments, w = new[name]
        where, arrays = zip(*blocks, strict=True)
        new[name] = [*moments, place(at, grads[which][0], part, arrays, where, w)]

    def send(n):
        which, part = PARTS[n]
        own = update(which, part)
        return across(own), sibling(own)

    def settle(n, away, beside):
        which, part = PARTS[n]
        put(which, part, (on(True, False), beside))
        put(which, part, (on(False, True), away))
        put(which, part, (on(False, False), sibling(away)))

    def both_blocks(name, which):
        part = (0, 2, 2)
        own = update(name + "1", part)
        *moments, w = new[name]
        arrays = keep_wide2, far_wide2, weights[name][0], *far_moments[name]
        away, w = adam_far(at, factor, 1, which, *arrays, w)
        new[name] = [*moments, w]
        beside, last = sibling(own), sibling(away)
        put(name + "1", part, (on(True, False), beside), (on(False, False), last))

    sent = [send(n) for n in range(len(PARTS) - 2)]
    both_blocks("gate", 2)
    both_blocks("up", 3)
    for n, parts in enumerate(sent):
        settle(n, *parts)
    for n, parts in enumerate([send(n) for n in range(len(sent), len(PARTS))], len(sent)):
        settle(n, *parts)
    return tuple(new[name][i] for i in (2, 0, 1) for name in weights)


PARTS = [
    ("down1", (0, 1, 10)),
    ("down1", (1, 2, 10)),
    ("down1", (1, 5, 5)),
    ("gate0", (0, 2, 2)),
    ("up0", (0, 2, 2)),
    ("down0", (0, 3, 5)),
    ("down0", (3, 5, 5)),
]


def solution(mesh):
    tokens, whole, rows = P(("rep", "dp")), P(), P(None, "dp")

    return jax.shard_map(
        step,
        mesh=mesh,
        in_specs=(tokens,) * 2 + (whole,) * 3 + (rows,) * 6,
        out_specs=(P("rep"),) * 3 + (P("rep", "dp"),) * 6,
        check_vma=False,
    )
```

```python
import functools

import jax
import jax.numpy as jnp
from jax import lax
from jax.experimental import pallas as pl
from jax.experimental.pallas import tpu as pltpu
from jax.sharding import PartitionSpec as P

BF, F32 = jnp.bfloat16, jnp.float32
NN = (((1,), (0,)), ((), ()))
NT = (((1,), (1,)), ((), ()))
CHUNK = 256
TOKENS, UNITS = 1024, 512


def dot(a, b, dims):
    return lax.dot_general(a, b, dims, preferred_element_type=F32)


def params():
    return pltpu.CompilerParams(vmem_limit_bytes=67043328)


def cost(flops, nbytes):
    return pl.CostEstimate(flops=int(flops), bytes_accessed=int(nbytes), transcendentals=0)


def out(shape, dtype=BF):
    return jax.ShapeDtypeStruct(shape, dtype)


def once(shape, index):
    return pl.BlockSpec(shape, index, pipeline_mode=pl.Buffered(1))


def call(kernel, at, grid, in_specs, out_specs, out_shape, operands, flops, nbytes, scratch=(), **kw):
    return pl.pallas_call(
        kernel,
        grid_spec=pltpu.PrefetchScalarGridSpec(
            num_scalar_prefetch=1, grid=grid, in_specs=in_specs, out_specs=out_specs, scratch_shapes=scratch
        ),
        out_shape=out_shape,
        compiler_params=params(),
        cost_estimate=cost(flops, nbytes),
        **kw,
    )(at, *operands)


def sigmoid(x):
    return 0.5 * jnp.tanh(0.5 * x) + 0.5


def chunks(n, size=CHUNK):
    return [slice(at, min(at + size, n)) for at in range(0, n, size)]


def loop(n, size, body):
    lax.fori_loop(0, n, lambda i, _: body(pl.ds(pl.multiple_of(i * size, size), size)), None)


def norm(h, a, a_out):
    def rows(r):
        wide = h[r, :].astype(F32)
        scale = lax.rsqrt(jnp.mean(wide * wide, -1, keepdims=True) + 1e-6)
        a[r, :] = (wide * scale).astype(BF)
        a_out[:, r] = a[r, :].T

    loop(a.shape[0] // CHUNK, CHUNK, rows)


def only(a, n, axis):
    return jnp.where(lax.broadcasted_iota(jnp.int32, a.shape, axis) < n, a, jnp.zeros_like(a))


PIECES, EARLY = 5, 6


def copied(at, step, moments, early, late, held, in_sems, out_sems):
    cols = held.shape[2]
    n = 2 * PIECES

    def columns(block):
        return pl.ds(pl.multiple_of(block * cols, 128), cols)

    def came_in(p):
        return pltpu.make_async_copy(moments[0].at[1, :, columns(0)], held.at[p % 2], in_sems.at[p % 2])

    def went_out(p):
        return pltpu.make_async_copy(held.at[p % 2], early.at[:, columns(0)], out_sems.at[p % 2])

    pl.when((step >= 2) & (step < n + 2))(lambda: went_out(step).wait())
    for which in range(2):
        for rep in range(2):

            @pl.when((step >= which * PIECES) & (step < (which + 1) * PIECES) & (at[2] == rep))
            def _(source=moments[2 * which + rep], block=step - which * PIECES):
                pltpu.make_async_copy(source.at[1, :, columns(block)], held.at[step % 2], in_sems.at[step % 2]).start()

    before = step - 1
    pl.when((before >= 0) & (before < n))(lambda: came_in(before).wait())
    for low, high, target in ((0, EARLY, early), (EARLY, n, late)):

        @pl.when((before >= low) & (before < high))
        def _(target=target, block=before - low):
            pltpu.make_async_copy(held.at[before % 2], target.at[:, columns(block)], out_sems.at[before % 2]).start()


def first_kernel(at, x, wg, wu, wd, *refs, f):
    moments, (a_out, hid, s_out, q_out, h_out, early, late, a, units, total, *held) = refs[:4], refs[4:]
    i, j = pl.program_id(0), pl.program_id(1)
    left = f - j * UNITS
    copied(at, i * pl.num_programs(1) + j, moments, early, late, *held)

    @pl.when(j == 0)
    def _():
        norm(x, a, a_out)
        total[...] = jnp.zeros_like(total)

    for c in chunks(UNITS):
        gate, up = dot(a[...], wg[:, c], NN), dot(a[...], wu[:, c], NN)
        sig = sigmoid(gate)
        silu = gate * sig
        units[:, c] = only((silu * up).astype(BF), left - c.start, 1)
        hid[c, :] = units[:, c].T
        s_out[:, c] = silu
        q_out[:, c] = up * (sig + silu * (1 - sig))
    for c in chunks(total.shape[1]):
        total[:, c] += dot(units[...], only(wd[:, c], left, 0), NN)

    @pl.when(j == pl.num_programs(1) - 1)
    def _():
        def rows(r):
            h_out[r, :] = x[r, :] + total[r, :].astype(BF)

        loop(x.shape[0] // CHUNK, CHUNK, rows)


def first(at, x, w_gate, w_up, w_down, moments):
    m = moments[0]
    t, d = x.shape
    f = w_gate.shape[2]
    wide = pl.BlockSpec((TOKENS, UNITS), lambda i, j, at: (i, j))
    weight = pl.BlockSpec((None, d, UNITS), lambda i, j, at: (0, 0, j))
    state = pl.BlockSpec((TOKENS, d), lambda i, j, at: (i, 0))
    return call(
        functools.partial(first_kernel, f=f),
        at,
        (t // TOKENS, pl.cdiv(f, UNITS)),
        [state, weight, weight, pl.BlockSpec((None, UNITS, d), lambda i, j, at: (0, j, 0))]
        + [pl.BlockSpec(memory_space=pl.ANY)] * 4,
        [
            pl.BlockSpec((d, TOKENS), lambda i, j, at: (0, i)),
            pl.BlockSpec((UNITS, TOKENS), lambda i, j, at: (j, i)),
            wide,
            wide,
            state,
        ]
        + [pl.BlockSpec(memory_space=pl.ANY)] * 2,
        [out((d, t)), out((f, t)), out((t, f), F32), out((t, f), F32), out((t, d))]
        + [out((m.shape[1], n * f // PIECES), F32) for n in (EARLY, 2 * PIECES - EARLY)],
        (x, w_gate, w_up, w_down, *moments),
        6 * t * d * f,
        190e6,
        scratch=[
            pltpu.VMEM((TOKENS, d), BF),
            pltpu.VMEM((TOKENS, UNITS), BF),
            pltpu.VMEM((TOKENS, d), F32),
            pltpu.VMEM((2, m.shape[1], f // PIECES), F32),
            pltpu.SemaphoreType.DMA((2,)),
            pltpu.SemaphoreType.DMA((2,)),
        ],
    )


def second_units(a, dy, wg, wu, wd, hid, dgu, left):
    for c in chunks(UNITS):
        for r in chunks(a.shape[0], a.shape[0] // (1 if c.start == 0 else 4)):
            gate, up = dot(a[r, :], wg[:, c], NN), dot(a[r, :], wu[:, c], NN)
            back = dot(dy[r, :], wd[c, :], NT).astype(BF).astype(F32)
            sig = sigmoid(gate)
            silu = gate * sig
            hid[c, r] = (silu * up).astype(BF).T
            dgu[0, r, c] = only((back * (up * (sig + silu * (1 - sig)))).astype(BF), left - c.start, 1)
            dgu[1, r, c] = only((back * silu).astype(BF), left - c.start, 1)


def second_kernel(at, h, dy, wg, wu, wd, a_before, dgu_before, a_out, dgu, hid, a, *, f):
    j = pl.program_id(1)

    @pl.when(j == 0)
    def _():
        norm(h, a, a_out)

    second_units(a, dy, wg, wu, wd, hid, dgu, f - j * UNITS)


def second_back_kernel(at, h, dy, wg, wu, wd, a_out, dgu, hid, d_out, a, of_gate, of_up, *, f):
    j = pl.program_id(1)
    left = f - j * UNITS

    @pl.when(j == 0)
    def _():
        norm(h, a, a_out)
        of_gate[...] = jnp.zeros_like(of_gate)
        of_up[...] = jnp.zeros_like(of_up)

    second_units(a, dy, wg, wu, wd, hid, dgu, left)
    for c in chunks(of_gate.shape[1]):
        of_gate[:, c] += dot(dgu[0], only(wg[c, :], left, 1), NT)
        of_up[:, c] += dot(dgu[1], only(wu[c, :], left, 1), NT)

    @pl.when(j == pl.num_programs(1) - 1)
    def _():
        def rows(r):
            da = (of_gate[r, :].astype(BF) + of_up[r, :].astype(BF)).astype(F32)
            wide = h[r, :].astype(F32)
            scale = lax.rsqrt(jnp.mean(wide * wide, -1, keepdims=True) + 1e-6)
            along = jnp.mean(da * wide, -1, keepdims=True) * (scale * scale * scale)
            d_out[r, :] = dy[r, :] + (da * scale - wide * along).astype(BF)

        loop(h.shape[0] // CHUNK, CHUNK, rows)


def second(at, h, dy, w_gate, w_up, w_down, before=None):
    t, d = h.shape
    f = w_gate.shape[2]
    far = before is not None
    bt = TOKENS
    weight = pl.BlockSpec((None, d, UNITS), lambda i, j, at: (1, 0, j))
    state = pl.BlockSpec((bt, d), lambda i, j, at: (i, 0))
    which = (lambda at: 1 - at[0]) if far else (lambda at: at[0])
    in_specs = [state, state, weight, weight, pl.BlockSpec((None, UNITS, d), lambda i, j, at: (1, j, 0))]
    out_specs = [
        pl.BlockSpec((None, d, bt), lambda i, j, at: (which(at), 0, i)),
        pl.BlockSpec((None, 2, bt, UNITS), lambda i, j, at: (which(at), 0, i, j)),
        pl.BlockSpec((UNITS, bt), lambda i, j, at: (j, i)),
    ]
    shapes = [out((2, d, t)), out((2, 2, t, f)), out((f, t))]
    scratch = [pltpu.VMEM((bt, d), BF)]
    operands = [h, dy, w_gate, w_up, w_down]
    aliases = {}
    if far:
        aliases = {6: 0, 7: 1}
        in_specs += [pl.BlockSpec(memory_space=pl.ANY)] * 2
        operands += before
    else:
        out_specs.append(state)
        shapes.append(out((t, d)))
        scratch += [pltpu.VMEM((bt, d), F32)] * 2
    return pl.pallas_call(
        functools.partial(second_kernel if far else second_back_kernel, f=f),
        grid_spec=pltpu.PrefetchScalarGridSpec(
            num_scalar_prefetch=1,
            grid=(t // bt, pl.cdiv(f, UNITS)),
            in_specs=in_specs,
            out_specs=out_specs,
            scratch_shapes=scratch,
        ),
        out_shape=shapes,
        input_output_aliases=aliases,
        compiler_params=params(),
        cost_estimate=cost((6 if far else 10) * t * d * f, 130e6),
        name="second" if far else "second_back",
    )(at, *operands)


def on(x_same, core_same):
    def block(at):
        return 2 * (at[0] if x_same else 1 - at[0]) + (at[1] if core_same else 1 - at[1])

    return block


def hidden_back_kernel(at, w, d, s, q, one, two, dgu, theirs):
    for c in chunks(UNITS):
        back = dot(d[...], w[c, :], NT).astype(BF).astype(F32)
        dgu[1, :, c] = (back * s[:, c]).astype(BF)
        dgu[0, :, c] = (back * q[:, c]).astype(BF)
    left = jnp.concatenate([one[...], two[...]], 0)
    for which in range(2):
        theirs[which] = dot(left, dgu[which], NN).reshape(theirs.shape[1:]).astype(BF)


def hidden_back(at, w_down, d_h, s, q, a):
    t, d = d_h.shape
    f = s.shape[1]
    rows = a.shape[1]
    wide = pl.BlockSpec((t, UNITS), lambda j, at: (0, j))
    return call(
        hidden_back_kernel,
        at,
        (pl.cdiv(f, UNITS),),
        [
            pl.BlockSpec((None, UNITS, d), lambda j, at: (0, j, 0)),
            once((t, d), lambda j, at: (0, 0)),
            wide,
            wide,
            once((None, rows, t), lambda j, at: (on(False, False)(at), 0, 0)),
            once((None, rows, t), lambda j, at: (on(True, False)(at), 0, 0)),
        ],
        [pl.BlockSpec((2, t, UNITS), lambda j, at: (0, 0, j)), pl.BlockSpec((2, 2, rows, UNITS), lambda j, at: (0, 0, 0, j))],
        [out((2, t, f)), out((2, 2, rows, f))],
        (w_down, d_h, s, q, a, a),
        4 * t * d * f,
        160e6,
    )


def wide_kernel(at, one, two, right, got, send, keep):
    rows = one.shape[0]
    total = dot(jnp.concatenate([one[...], two[...]], 0), right[...], NN)
    total = total + got[...].reshape(total.shape).astype(F32)
    send[...], keep[...] = total[:rows].astype(BF), total[rows:]


def grad_wide(at, left, right, one, two, got):
    rows, t = left.shape[1:]
    f = right.shape[2]
    bn = 768
    return call(
        wide_kernel,
        at,
        (2, pl.cdiv(f, bn)),
        [once((None, rows, t), lambda w, j, at, b=b: (b(at), 0, 0)) for b in (one, two)]
        + [pl.BlockSpec((None, t, bn), lambda w, j, at: (w, 0, j)), pl.BlockSpec((None, 2, rows, bn), lambda w, j, at: (w, 0, 0, j))],
        [pl.BlockSpec((None, rows, bn), lambda w, j, at: (w, 0, j))] * 2,
        [out((2, rows, f)), out((2, rows, f), F32)],
        (left, left, right, got),
        8 * rows * t * f,
        60e6,
    )


def whole_kernel(at, left0, left1, right0, right1, send, keep, total):
    total[...] = (dot(left0[...], right0[...], NN) + dot(left1[...], right1[...], NN)).reshape(total.shape)
    send[...], keep[...] = total[1 - at[1]].astype(BF), total[at[1]]


def grad_whole(at, left, right):
    d, t = left.shape[1:]
    f = right.shape[3]
    rows, bn = d // 4, 768
    same = pl.BlockSpec((None, rows, bn), lambda w, j, at: (w, 0, j))

    def half(w, at):
        return jnp.where(w < 2, at[0], 1 - at[0])

    return call(
        whole_kernel,
        at,
        (4, pl.cdiv(f, bn)),
        [pl.BlockSpec((None, 2 * rows, t), lambda w, j, at, x=x: (x, half(w, at), 0)) for x in range(2)]
        + [pl.BlockSpec((None, None, t, bn), lambda w, j, at, x=x: (x, w % 2, 0, j)) for x in range(2)],
        [same, same],
        [out((4, rows, f)), out((4, rows, f), F32)],
        (left, left, right, right),
        8 * d * t * f,
        120e6,
        scratch=[pltpu.VMEM((2, rows, bn), F32)],
    )


def tall_kernel(at, *refs, terms, add, keeps):
    operands, rest = refs[: 2 * terms], refs[2 * terms :]
    half = pl.num_programs(0) // 2
    total = 0
    for left, right in zip(operands[::2], operands[1::2], strict=True):
        total = total + dot(left[...], right[...], NN)
    if add:
        total = total + rest[0][...].astype(F32)
    if not keeps:
        rest[-1][...] = total.astype(BF)
        return

    @pl.when(pl.program_id(0) < half)
    def _():
        rest[-2][...] = total.astype(BF)

    @pl.when(pl.program_id(0) >= half)
    def _():
        rest[-1][...] = total


def grad_tall(at, pairs, one, two, got=None, keeps=True, half=4):
    rows, t = pairs[0][0].shape[1:]
    d = pairs[0][1].shape[1]
    bm = rows // half
    in_specs, operands = [], []
    for left, right in pairs:
        in_specs += [
            pl.BlockSpec((None, bm, t), lambda j, at: (jnp.where(j < half, one(at), two(at)), j % half, 0)),
            once(right.shape, lambda j, at: (0, 0)),
        ]
        operands += [left, right]
    if got is not None:
        in_specs.append(pl.BlockSpec((None, bm, d), lambda j, at: (j // half, j % half, 0)))
        operands.append(got)
    if keeps:
        out_specs = [pl.BlockSpec((bm, d), lambda j, at: (jnp.minimum(j, half - 1), 0)), pl.BlockSpec((bm, d), lambda j, at: (jnp.maximum(j - half, 0), 0))]
        shapes = [out((rows, d)), out((rows, d), F32)]
    else:
        out_specs = [pl.BlockSpec((None, bm, d), lambda j, at: (j // half, j % half, 0))]
        shapes = [out((2, rows, d))]
    return call(
        functools.partial(tall_kernel, terms=len(pairs), add=got is not None, keeps=keeps),
        at,
        (2 * half,),
        in_specs,
        out_specs,
        shapes,
        operands,
        4 * rows * t * d * len(pairs),
        60e6,
    )


def squares_kernel(*refs, shapes, n):
    arrays, o, held, sems = refs[: len(shapes)], refs[len(shapes)], refs[len(shapes) + 1 : -1], refs[-1]

    def copies(k, i):
        rows = shapes[k][1] // n
        r = pl.ds(i * rows, rows)
        return pltpu.make_async_copy(arrays[k].at[pl.ds(0, shapes[k][0]), r], held[k].at[:, r], sems.at[k, i])

    everything = [(k, i) for k in range(0, len(shapes), 2) for i in range(n)]
    for k, i in everything:
        copies(k, i).start()
        copies(k + 1, i).start()
    o[...] = jnp.zeros_like(o)
    for k, i in everything:
        copies(k, i).wait()
        copies(k + 1, i).wait()
        rows = shapes[k][1] // n

        def add(t, _, k=k, start=i * rows, size=rows // 16):
            r = pl.ds(pl.multiple_of(start + t % size * 16, 16), 16)
            g = (held[k][t // size, r, :] + held[k + 1][t // size, r, :].astype(F32)).astype(BF).astype(F32)
            g = jnp.sum((g * g).reshape(-1, 8, g.shape[-1]), 0)
            o[...] += sum(g[:, c] for c in chunks(g.shape[1], 128))

        lax.fori_loop(0, shapes[k][0] * (rows // 16), add, None)


def sum_of_squares(*pairs):
    n = 5
    arrays = [a for pair in pairs for a in pair[:2]]
    shapes = [(pair[2], *a.shape[1:]) for pair in pairs for a in pair[:2]]
    held = [pltpu.VMEM(shape, a.dtype) for shape, a in zip(shapes, arrays, strict=True)]
    return pl.pallas_call(
        functools.partial(squares_kernel, shapes=shapes, n=n),
        in_specs=[pl.BlockSpec(memory_space=pl.ANY)] * len(arrays),
        out_specs=pl.BlockSpec(memory_space=pltpu.VMEM),
        out_shape=out((8, 128), F32),
        scratch_shapes=[*held, pltpu.SemaphoreType.DMA((len(arrays), n))],
        compiler_params=params(),
        cost_estimate=cost(1e9, 4e6 * len(arrays)),
        name="squares",
    )(*arrays)


def updated(g, w, m, v):
    m = 0.9 * m + 0.1 * g
    v = 0.95 * v + 0.05 * g * g
    wide = w.astype(F32)
    return (wide - 0.02 * (m * lax.rsqrt(v + 1e-8) + 0.1 * wide)).astype(BF), m, v


def gradient(factor, keep, far, r):
    return (keep[r, :] + far[r, :].astype(F32)).astype(BF).astype(F32) * factor[0]


def adam_kernel(at, factor, keep, far, w, m, v, *rest):
    w_out, m_out, v_out, w_new = rest[-4:]

    def rows(r):
        w_out[r, :], m_out[r, :], v_out[r, :] = updated(gradient(factor, keep, far, r), w[r, :], m[r, :], v[r, :])
        w_new[r, :] = w_out[r, :]

    loop(w.shape[0] // 16, 16, rows)


def adam(at, factor, layer, which, part, keep, far, w, m, v, before):
    rows, cols = keep.shape[1:]
    low, high, n = part
    br = rows // n
    own = pl.BlockSpec((None, br, cols), lambda i, at: (layer, low + i, 0))
    grad = pl.BlockSpec((None, br, cols), lambda i, at: (which, low + i, 0))
    there = pl.BlockSpec((None, br, cols), lambda i, at: (layer, (2 * at[0] + at[1]) * n + low + i, 0))
    return call(
        adam_kernel,
        at,
        (high - low,),
        [pl.BlockSpec(memory_space=pltpu.SMEM), grad, grad, there, own, own] + [pl.BlockSpec(memory_space=pl.ANY)] * len(before),
        [pl.BlockSpec((br, cols), lambda i, at: (i, 0)), own, own, there],
        [out((br * (high - low), cols)), out(m.shape, F32), out(v.shape, F32), out(w.shape)],
        [factor, keep, far, w, m, v, *before],
        1e9,
        6e6 * (high - low),
        input_output_aliases={7: 1, 8: 2, 9: 3} if before else {},
    )


def adam_far_kernel(at, factor, keep, far, w, *refs, start):
    *moments, before, w_out, w_new = refs
    first = at[2] == 0

    def update(crossed, handed):
        def rows(r):
            m, v = jnp.where(first, crossed[r, :], handed[r, :]), jnp.where(first, handed[r, :], crossed[r, :])
            w_out[r, :], _, _ = updated(gradient(factor, keep, far, r), w[r, :], m, v)
            w_new[r, :] = w_out[r, :]

        loop(w.shape[0] // 32, 32, rows)

    if len(moments) == 2:
        update(*moments)
    else:
        early = pl.program_id(1) + start < EARLY
        pl.when(early)(lambda: update(*moments[:2]))
        pl.when(~early)(lambda: update(*moments[2:]))


def adam_far(at, factor, layer, which, start, keep, far, w, moments, before):
    rows, cols = keep.shape[1:]
    n = 2
    br, bc = rows // n, cols // PIECES
    grad = pl.BlockSpec((None, br, bc), lambda i, j, at: (which, i, j))
    flat = pl.BlockSpec((br, bc), lambda i, j, at: (i, j))
    there = pl.BlockSpec((None, br, bc), lambda i, j, at: (layer, (2 * (1 - at[0]) + at[1]) * n + i, j))
    early = pl.BlockSpec((br, bc), lambda i, j, at: (i, jnp.minimum(j + start, EARLY - 1)))
    late = pl.BlockSpec((br, bc), lambda i, j, at: (i, jnp.maximum(j + start - EARLY, 0)))
    specs = ([early] * 2 if start < EARLY else []) + ([late] * 2 if start + PIECES > EARLY else [])
    moments = moments[: len(specs)]
    return call(
        functools.partial(adam_far_kernel, start=start),
        at,
        (n, PIECES),
        [pl.BlockSpec(memory_space=pltpu.SMEM), grad, grad, there, *specs, pl.BlockSpec(memory_space=pl.ANY)],
        [flat, there],
        [out((rows, cols)), out(w.shape)],
        [factor, keep, far, w, *moments, before],
        1e9,
        30e6,
        input_output_aliases={5 + len(specs): 1},
    )


def place_kernel(at, *refs, count):
    for n in range(count):
        pl.when(pl.program_id(0) == n)(functools.partial(lambda n: refs[-1].__setitem__(..., refs[n][...]), n))


def place(at, layer, part, blocks, wheres, before):
    low, high, n = part
    k = high - low
    cols = blocks[0].shape[1]
    br = blocks[0].shape[0] // k

    def spec(n):
        return pl.BlockSpec((br, cols), lambda i, j, at: (jnp.where(i < n, 0, jnp.where(i > n, k - 1, j)), 0))

    def where(i, j, at):
        b = wheres[0](at)
        for k, w in enumerate(wheres[1:], 1):
            b = jnp.where(i == k, w(at), b)
        return layer, b * n + low + j, 0

    return call(
        functools.partial(place_kernel, count=len(blocks)),
        at,
        (len(blocks), k),
        [spec(n) for n in range(len(blocks))] + [pl.BlockSpec(memory_space=pl.ANY)],
        pl.BlockSpec((None, br, cols), where),
        out(before.shape),
        [*blocks, before],
        1e9,
        1.2e6 * k * len(blocks),
        input_output_aliases={1 + len(blocks): 0},
    )


def after(value, *others):
    return lax.optimization_barrier((value, *others))[0]


ACROSS = [(0, 2), (2, 0), (1, 3), (3, 1)]
SIBLING = [(0, 1), (1, 0), (2, 3), (3, 2)]


def across(a):
    return lax.ppermute(a, "dp", ACROSS)


def sibling(a):
    return lax.ppermute(a, "dp", SIBLING)


def step(x, dy, w_gate, w_up, w_down, m_gate, m_up, m_down, v_gate, v_up, v_down):
    dp = lax.axis_index("dp")
    at = jnp.stack([dp // 2, dp % 2, lax.axis_index("rep")]).astype(jnp.int32)
    x, dy = x[0], dy[0]
    d, f = w_gate.shape[1:]

    def blocks(a):
        return a.reshape(4, a.shape[0] // 4, a.shape[1])

    dy_far = across(dy)
    moments = m_gate, v_gate, m_up, v_up
    a1, hid1, s1, q1, h1, early, late = first(at, x, w_gate, w_up, w_down, moments)
    h1_far = across(h1)

    def brought(half):
        crossed = across(half)
        return crossed, lax.ppermute(crossed, "rep", [(0, 1), (1, 0)])

    far_moments = (*brought(early), *brought(late))
    a2, dgu2, hid2, d1 = second(at, h1, dy, w_gate, w_up, w_down)

    dgu1, theirs = hidden_back(at, w_down, d1, s1, q1, blocks(a1))
    got_wide = sibling(theirs)
    pairs = [(blocks(hid1), after(d1, theirs))]
    (theirs,) = grad_tall(at, pairs, on(False, False), on(True, False), keeps=False)
    got_down = sibling(theirs)
    got_wide = after(got_wide, theirs)
    send, keep_wide1 = grad_wide(at, blocks(a1), dgu1, on(False, True), on(True, True), got_wide)
    far_wide1 = across(send)
    got_down = after(got_down, keep_wide1)
    send, keep_down1 = grad_tall(at, pairs, on(False, True), on(True, True), got_down, half=7)
    far_down1 = across(send)

    h1_far = after(h1_far, keep_down1)
    a2, dgu2, hid2f = second(at, h1_far, dy_far, w_gate, w_up, w_down, [a2, dgu2])
    send, keep_wide2 = grad_whole(at, a2, dgu2)
    far_wide2 = sibling(send)
    pairs = [(blocks(hid2), dy), (blocks(after(hid2f, keep_wide2)), dy_far)]
    send, keep_down2 = grad_tall(at, pairs, on(True, False), on(True, True), half=7)
    far_down2 = sibling(send)
    keep_down1, far_down1, keep_down2, far_down2 = (a[None] for a in (keep_down1, far_down1, keep_down2, far_down2))
    squares = sum_of_squares((keep_wide1, far_wide1, 2), (keep_down1, far_down1, 1), (keep_wide2, far_wide2, 2))
    far_down2 = after(far_down2, squares)
    squares = squares + sum_of_squares((keep_down2, far_down2, 1))
    squares = squares + sibling(squares)
    squares = squares + across(squares)
    factor = jnp.minimum(1.0, 0.5 * lax.rsqrt(jnp.sum(squares) / (6 * d * f) + 1e-30)).reshape(1)

    weights = {"gate": (w_gate, m_gate, v_gate), "up": (w_up, m_up, v_up), "down": (w_down, m_down, v_down)}
    grads = {
        "gate1": (1, 0, keep_wide2, far_wide2),
        "up1": (1, 1, keep_wide2, far_wide2),
        "down1": (1, 0, keep_down2, far_down2),
        "gate0": (0, 0, keep_wide1, far_wide1),
        "up0": (0, 1, keep_wide1, far_wide1),
        "down0": (0, 0, keep_down1, far_down1),
    }
    new = dict.fromkeys(weights, ())

    def update(which, part):
        name = which[:-1]
        own, *new[name] = adam(at, factor, *grads[which][:2], part, *grads[which][2:], *weights[name], new[name])
        return own

    def put(which, part, *blocks):
        name = which[:-1]
        *moments, w = new[name]
        where, arrays = zip(*blocks, strict=True)
        new[name] = [*moments, place(at, grads[which][0], part, arrays, where, w)]

    def send(n):
        which, part = PARTS[n]
        own = update(which, part)
        return across(own), sibling(own)

    def settle(sent):
        for n, (_, beside) in sent.items():
            put(*PARTS[n], (on(True, False), beside))
        for n, (away, _) in sent.items():
            put(*PARTS[n], (on(False, True), away))
            put(*PARTS[n], (on(False, False), sibling(away)))

    def both_blocks(name, which):
        part = (0, 2, 2)
        own = update(name + "1", part)
        *moments, w = new[name]
        arrays = keep_wide2, far_wide2, weights[name][0], far_moments
        away, w = adam_far(at, factor, 1, which, (which - 2) * PIECES, *arrays, w)
        new[name] = [*moments, w]
        beside, last = sibling(own), sibling(away)
        put(name + "1", part, (on(True, False), beside), (on(False, False), last))

    sent = {n: send(n) for n in range(len(PARTS) - 2)}
    both_blocks("gate", 2)
    both_blocks("up", 3)
    settle(sent)
    settle({n: send(n) for n in range(len(sent), len(PARTS))})
    return tuple(new[name][i] for i in (2, 0, 1) for name in weights)


PARTS = [
    ("down1", (0, 1, 10)),
    ("down1", (1, 2, 10)),
    ("down1", (1, 5, 5)),
    ("gate0", (0, 2, 2)),
    ("up0", (0, 2, 2)),
    ("down0", (0, 3, 5)),
    ("down0", (3, 5, 5)),
]


def solution(mesh):
    tokens, whole, rows = P(("rep", "dp")), P(), P(None, "dp")

    return jax.shard_map(
        step,
        mesh=mesh,
        in_specs=(tokens,) * 2 + (whole,) * 3 + (rows,) * 6,
        out_specs=(P("rep"),) * 3 + (P("rep", "dp"),) * 6,
        check_vma=False,
    )
```

```python
import functools
import math

import jax
import jax.numpy as jnp
from jax import lax
from jax.experimental import pallas as pl
from jax.experimental.pallas import tpu as pltpu
from jax.sharding import PartitionSpec as P

BF, F32 = jnp.bfloat16, jnp.float32
NN = (((1,), (0,)), ((), ()))
NT = (((1,), (1,)), ((), ()))
CHUNK = 256
TOKENS, UNITS = 1024, 512


def dot(a, b, dims):
    return lax.dot_general(a, b, dims, preferred_element_type=F32)


def params():
    return pltpu.CompilerParams(vmem_limit_bytes=67043328)


def cost(flops, nbytes):
    return pl.CostEstimate(flops=int(flops), bytes_accessed=int(nbytes), transcendentals=0)


def out(shape, dtype=BF):
    return jax.ShapeDtypeStruct(shape, dtype)


def once(shape, index):
    return pl.BlockSpec(shape, index, pipeline_mode=pl.Buffered(1))


def call(kernel, at, grid, in_specs, out_specs, out_shape, operands, flops, nbytes, scratch=(), **kw):
    return pl.pallas_call(
        kernel,
        grid_spec=pltpu.PrefetchScalarGridSpec(
            num_scalar_prefetch=1, grid=grid, in_specs=in_specs, out_specs=out_specs, scratch_shapes=scratch
        ),
        out_shape=out_shape,
        compiler_params=params(),
        cost_estimate=cost(flops, nbytes),
        **kw,
    )(at, *operands)


def sigmoid(x):
    return 0.5 * jnp.tanh(0.5 * x) + 0.5


def chunks(n, size=CHUNK):
    return [slice(at, min(at + size, n)) for at in range(0, n, size)]


def loop(n, size, body):
    lax.fori_loop(0, n, lambda i, _: body(pl.ds(pl.multiple_of(i * size, size), size)), None)


def norm(h, a, a_out):
    def rows(r):
        wide = h[r, :].astype(F32)
        scale = lax.rsqrt(jnp.mean(wide * wide, -1, keepdims=True) + 1e-6)
        a[r, :] = (wide * scale).astype(BF)
        a_out[:, r] = a[r, :].T

    loop(a.shape[0] // CHUNK, CHUNK, rows)


def unless_first(total):
    return jnp.where(pl.program_id(1) == 0, 0.0, total)


def only(a, n, axis):
    return jnp.where(lax.broadcasted_iota(jnp.int32, a.shape, axis) < n, a, jnp.zeros_like(a))


PIECES, OF_UP, EARLY = 5, 4, 6


def copied(at, step, moments, early, late, held, in_sems, out_sems):
    cols = held.shape[2]
    n = PIECES + OF_UP

    def columns(block):
        return pl.ds(pl.multiple_of(block * cols, 128), cols)

    def came_in(p):
        return pltpu.make_async_copy(moments[0].at[1, :, columns(0)], held.at[p % 2], in_sems.at[p % 2])

    def went_out(p):
        return pltpu.make_async_copy(held.at[p % 2], early.at[:, columns(0)], out_sems.at[p % 2])

    pl.when((step >= 2) & (step < n + 2))(lambda: went_out(step).wait())
    for which in range(2):
        for rep in range(2):

            @pl.when((step >= which * PIECES) & (step < min((which + 1) * PIECES, n)) & (at[2] == rep))
            def _(source=moments[2 * which + rep], block=step - which * PIECES):
                pltpu.make_async_copy(source.at[1, :, columns(block)], held.at[step % 2], in_sems.at[step % 2]).start()

    before = step - 1
    pl.when((before >= 0) & (before < n))(lambda: came_in(before).wait())
    for low, high, target in ((0, EARLY, early), (EARLY, n, late)):

        @pl.when((before >= low) & (before < high))
        def _(target=target, block=before - low):
            pltpu.make_async_copy(held.at[before % 2], target.at[:, columns(block)], out_sems.at[before % 2]).start()


def first_kernel(at, x, wg, wu, wd, *refs, f):
    moments, (a_out, hid, s_out, q_out, h_out, early, late, a, units, total, *held) = refs[:4], refs[4:]
    i, j = pl.program_id(0), pl.program_id(1)
    left = f - j * UNITS
    copied(at, i * pl.num_programs(1) + j, moments, early, late, *held)

    @pl.when(j == 0)
    def _():
        norm(x, a, a_out)

    for c in chunks(UNITS):
        for r in chunks(a.shape[0]):
            gate, up = dot(a[r, :], wg[:, c], NN), dot(a[r, :], wu[:, c], NN)
            sig = sigmoid(gate)
            silu = gate * sig
            units[r, c] = only((silu * up).astype(BF), left - c.start, 1)
            hid[c, r] = units[r, c].T
            s_out[r, c] = silu
            q_out[r, c] = up * (sig + silu * (1 - sig))
    for c in chunks(total.shape[1]):
        total[:, c] = unless_first(total[:, c]) + dot(units[...], only(wd[:, c], left, 0), NN)

    @pl.when(j == pl.num_programs(1) - 1)
    def _():
        def rows(r):
            h_out[r, :] = x[r, :] + total[r, :].astype(BF)

        loop(x.shape[0] // CHUNK, CHUNK, rows)


def first(at, x, w_gate, w_up, w_down, moments):
    m = moments[0]
    t, d = x.shape
    f = w_gate.shape[2]
    n = pl.cdiv(f, UNITS)
    wide = pl.BlockSpec((None, TOKENS, UNITS), lambda i, j, at: (j, i, 0))
    weight = pl.BlockSpec((None, d, UNITS), lambda i, j, at: (0, 0, j))
    state = pl.BlockSpec((TOKENS, d), lambda i, j, at: (i, 0))
    return call(
        functools.partial(first_kernel, f=f),
        at,
        (t // TOKENS, pl.cdiv(f, UNITS)),
        [state, weight, weight, pl.BlockSpec((None, UNITS, d), lambda i, j, at: (0, j, 0))]
        + [pl.BlockSpec(memory_space=pl.ANY)] * 4,
        [
            pl.BlockSpec((d, TOKENS), lambda i, j, at: (0, i)),
            pl.BlockSpec((UNITS, TOKENS), lambda i, j, at: (j, i)),
            wide,
            wide,
            state,
        ]
        + [pl.BlockSpec(memory_space=pl.ANY)] * 2,
        [out((d, t)), out((f, t)), *[out((n, t, UNITS), F32)] * 2, out((t, d))]
        + [out((m.shape[1], n * f // PIECES), F32) for n in (EARLY, PIECES + OF_UP - EARLY)],
        (x, w_gate, w_up, w_down, *moments),
        6 * t * d * f,
        190e6,
        scratch=[
            pltpu.VMEM((TOKENS, d), BF),
            pltpu.VMEM((TOKENS, UNITS), BF),
            pltpu.VMEM((TOKENS, d), F32),
            pltpu.VMEM((2, m.shape[1], f // PIECES), F32),
            pltpu.SemaphoreType.DMA((2,)),
            pltpu.SemaphoreType.DMA((2,)),
        ],
    )


def second_units(a, dy, wg, wu, wd, hid, dgu, left):
    for c in chunks(hid.shape[0]):
        for r in chunks(a.shape[0]):
            gate, up = dot(a[r, :], wg[:, c], NN), dot(a[r, :], wu[:, c], NN)
            back = dot(dy[r, :], wd[c, :], NT).astype(BF).astype(F32)
            sig = sigmoid(gate)
            silu = gate * sig
            hid[c, r] = (silu * up).astype(BF).T
            dgu[0, r, c] = only((back * (up * (sig + silu * (1 - sig)))).astype(BF), left - c.start, 1)
            dgu[1, r, c] = only((back * silu).astype(BF), left - c.start, 1)


def second_kernel(at, h, dy, wg, wu, wd, a_before, dgu_before, a_out, dgu, hid, a, *, f):
    j = pl.program_id(1)

    @pl.when(j == 0)
    def _():
        norm(h, a, a_out)

    second_units(a, dy, wg, wu, wd, hid, dgu, f - j * hid.shape[0])


def second_back_kernel(at, h, dy, wg, wu, wd, a_out, dgu, hid, d_out, a, of_gate, of_up, *, f):
    j = pl.program_id(1)
    left = f - j * UNITS

    @pl.when(j == 0)
    def _():
        norm(h, a, a_out)

    second_units(a, dy, wg, wu, wd, hid, dgu, left)
    for c in chunks(of_gate.shape[1]):
        of_gate[:, c] = unless_first(of_gate[:, c]) + dot(dgu[0], only(wg[c, :], left, 1), NT)
        of_up[:, c] = unless_first(of_up[:, c]) + dot(dgu[1], only(wu[c, :], left, 1), NT)

    @pl.when(j == pl.num_programs(1) - 1)
    def _():
        def rows(r):
            da = (of_gate[r, :].astype(BF) + of_up[r, :].astype(BF)).astype(F32)
            wide = h[r, :].astype(F32)
            scale = lax.rsqrt(jnp.mean(wide * wide, -1, keepdims=True) + 1e-6)
            along = jnp.mean(da * wide, -1, keepdims=True) * (scale * scale * scale)
            d_out[r, :] = dy[r, :] + (da * scale - wide * along).astype(BF)

        loop(h.shape[0] // CHUNK, CHUNK, rows)


def second(at, h, dy, w_gate, w_up, w_down, before=None):
    t, d = h.shape
    f = w_gate.shape[2]
    far = before is not None
    bt, bf = TOKENS, UNITS
    weight = pl.BlockSpec((None, d, bf), lambda i, j, at: (1, 0, j))
    state = pl.BlockSpec((bt, d), lambda i, j, at: (i, 0))
    which = (lambda at: 1 - at[0]) if far else (lambda at: at[0])
    in_specs = [state, state, weight, weight, pl.BlockSpec((None, bf, d), lambda i, j, at: (1, j, 0))]
    out_specs = [
        pl.BlockSpec((None, d, bt), lambda i, j, at: (which(at), 0, i)),
        pl.BlockSpec((None, 2, bt, bf), lambda i, j, at: (which(at), 0, i, j)),
        pl.BlockSpec((bf, bt), lambda i, j, at: (j, i)),
    ]
    shapes = [out((2, d, t)), out((2, 2, t, f)), out((f, t))]
    scratch = [pltpu.VMEM((bt, d), BF)]
    operands = [h, dy, w_gate, w_up, w_down]
    aliases = {}
    if far:
        aliases = {6: 0, 7: 1}
        in_specs += [pl.BlockSpec(memory_space=pl.ANY)] * 2
        operands += before
    else:
        out_specs.append(state)
        shapes.append(out((t, d)))
        scratch += [pltpu.VMEM((bt, d), F32)] * 2
    return pl.pallas_call(
        functools.partial(second_kernel if far else second_back_kernel, f=f),
        grid_spec=pltpu.PrefetchScalarGridSpec(
            num_scalar_prefetch=1,
            grid=(t // bt, pl.cdiv(f, bf)),
            in_specs=in_specs,
            out_specs=out_specs,
            scratch_shapes=scratch,
        ),
        out_shape=shapes,
        input_output_aliases=aliases,
        compiler_params=params(),
        cost_estimate=cost((6 if far else 10) * t * d * f, 130e6),
        name="second" if far else "second_back",
    )(at, *operands)


def on(x_same, core_same):
    def block(at):
        return 2 * (at[0] if x_same else 1 - at[0]) + (at[1] if core_same else 1 - at[1])

    return block


def hidden_back_kernel(at, w, d, s, q, one, two, dgu, theirs):
    for r in chunks(d.shape[0]):
        back = dot(d[r, :], w[...], NT).astype(BF).astype(F32)
        dgu[1, r, :] = (back * s[r, :]).astype(BF)
        dgu[0, r, :] = (back * q[r, :]).astype(BF)
    left = jnp.concatenate([one[...], two[...]], 0)
    for which in range(2):
        theirs[which] = dot(left, dgu[which], NN).reshape(theirs.shape[1:]).astype(BF)


def hidden_back(at, w_down, d_h, s, q, a):
    t, d = d_h.shape
    f = w_down.shape[1]
    rows, bf = a.shape[1], UNITS
    wide = pl.BlockSpec((None, t, bf), lambda j, at: (j, 0, 0))
    return call(
        hidden_back_kernel,
        at,
        (pl.cdiv(f, bf),),
        [
            pl.BlockSpec((None, bf, d), lambda j, at: (0, j, 0)),
            once((t, d), lambda j, at: (0, 0)),
            wide,
            wide,
            once((None, rows, t), lambda j, at: (on(False, False)(at), 0, 0)),
            once((None, rows, t), lambda j, at: (on(True, False)(at), 0, 0)),
        ],
        [pl.BlockSpec((2, t, bf), lambda j, at: (0, 0, j)), pl.BlockSpec((2, 2, rows, bf), lambda j, at: (0, 0, 0, j))],
        [out((2, t, f)), out((2, 2, rows, f))],
        (w_down, d_h, s, q, a, a),
        4 * t * d * f,
        160e6,
    )


def wide_kernel(at, one, two, right, got, send, keep):
    rows = one.shape[0]
    total = dot(jnp.concatenate([one[...], two[...]], 0), right[...], NN)
    total = total + got[...].reshape(total.shape).astype(F32)
    send[...], keep[...] = total[:rows].astype(BF), total[rows:]


def grad_wide(at, left, right, one, two, got):
    rows, t = left.shape[1:]
    f = right.shape[2]
    bn = 1536
    return call(
        wide_kernel,
        at,
        (2, pl.cdiv(f, bn)),
        [once((None, rows, t), lambda w, j, at, b=b: (b(at), 0, 0)) for b in (one, two)]
        + [pl.BlockSpec((None, t, bn), lambda w, j, at: (w, 0, j)), pl.BlockSpec((None, 2, rows, bn), lambda w, j, at: (w, 0, 0, j))],
        [pl.BlockSpec((None, rows, bn), lambda w, j, at: (w, 0, j))] * 2,
        [out((2, rows, f)), out((2, rows, f), F32)],
        (left, left, right, got),
        8 * rows * t * f,
        60e6,
    )


def whole_kernel(at, left0, left1, right0, right1, send, keep, total, *, last):
    needed = (pl.program_id(0) < 3) | (pl.program_id(1) < last)

    @pl.when(needed)
    def _():
        total[...] = (dot(left0[...], right0[...], NN) + dot(left1[...], right1[...], NN)).reshape(total.shape)
        send[...], keep[...] = total[1 - at[1]].astype(BF), total[at[1]]

    @pl.when(~needed)
    def _():
        send[...], keep[...] = jnp.zeros_like(send), jnp.zeros_like(keep)


def grad_whole(at, left, right):
    d, t = left.shape[1:]
    f = right.shape[3]
    rows, bn = d // 4, 768
    same = pl.BlockSpec((None, rows, bn), lambda w, j, at: (w, 0, j))

    def half(w, at):
        return jnp.where(w < 2, at[0], 1 - at[0])

    return call(
        functools.partial(whole_kernel, last=pl.cdiv(f * OF_UP // PIECES, bn)),
        at,
        (4, pl.cdiv(f, bn)),
        [pl.BlockSpec((None, 2 * rows, t), lambda w, j, at, x=x: (x, half(w, at), 0)) for x in range(2)]
        + [pl.BlockSpec((None, None, t, bn), lambda w, j, at, x=x: (x, w % 2, 0, j)) for x in range(2)],
        [same, same],
        [out((4, rows, f)), out((4, rows, f), F32)],
        (left, left, right, right),
        8 * d * t * f,
        120e6,
        scratch=[pltpu.VMEM((2, rows, bn), F32)],
    )


def tall_kernel(at, *refs, terms, add, keeps):
    operands, rest = refs[: 2 * terms], refs[2 * terms :]
    half = pl.num_programs(0) // 2
    total = 0
    for left, right in zip(operands[::2], operands[1::2], strict=True):
        total = total + dot(left[...], right[...], NN)
    if add:
        total = total + rest[0][...].astype(F32)
    if not keeps:
        rest[-1][...] = total.astype(BF)
        return

    @pl.when(pl.program_id(0) < half)
    def _():
        rest[-2][...] = total.astype(BF)

    @pl.when(pl.program_id(0) >= half)
    def _():
        rest[-1][...] = total


def grad_tall(at, pairs, one, two, got=None, keeps=True, half=4):
    rows, t = pairs[0][0].shape[1:]
    d = pairs[0][1].shape[1]
    bm = rows // half
    in_specs, operands = [], []
    for left, right in pairs:
        in_specs += [
            pl.BlockSpec((None, bm, t), lambda j, at: (jnp.where(j < half, one(at), two(at)), j % half, 0)),
            once(right.shape, lambda j, at: (0, 0)),
        ]
        operands += [left, right]
    if got is not None:
        in_specs.append(pl.BlockSpec((None, bm, d), lambda j, at: (j // half, j % half, 0)))
        operands.append(got)
    if keeps:
        out_specs = [pl.BlockSpec((bm, d), lambda j, at: (jnp.minimum(j, half - 1), 0)), pl.BlockSpec((bm, d), lambda j, at: (jnp.maximum(j - half, 0), 0))]
        shapes = [out((rows, d)), out((rows, d), F32)]
    else:
        out_specs = [pl.BlockSpec((None, bm, d), lambda j, at: (j // half, j % half, 0))]
        shapes = [out((2, rows, d))]
    return call(
        functools.partial(tall_kernel, terms=len(pairs), add=got is not None, keeps=keeps),
        at,
        (2 * half,),
        in_specs,
        out_specs,
        shapes,
        operands,
        4 * rows * t * d * len(pairs),
        60e6,
    )


def squares_kernel(*refs, shapes, n):
    arrays, o, held, sems = refs[: len(shapes)], refs[len(shapes)], refs[len(shapes) + 1 : -1], refs[-1]

    def copies(k, i):
        rows = shapes[k][1] // n
        r = pl.ds(i * rows, rows)
        return pltpu.make_async_copy(arrays[k].at[pl.ds(0, shapes[k][0]), r], held[k].at[:, r], sems.at[k, i])

    everything = [(k, i) for k in range(0, len(shapes), 2) for i in range(n)]
    for k, i in everything:
        copies(k, i).start()
        copies(k + 1, i).start()
    o[...] = jnp.zeros_like(o)
    for k, i in everything:
        copies(k, i).wait()
        copies(k + 1, i).wait()
        rows = shapes[k][1] // n

        def add(t, _, k=k, start=i * rows, size=rows // 16):
            r = pl.ds(pl.multiple_of(start + t % size * 16, 16), 16)
            g = (held[k][t // size, r, :] + held[k + 1][t // size, r, :].astype(F32)).astype(BF).astype(F32)
            g = jnp.sum((g * g).reshape(-1, 8, g.shape[-1]), 0)
            o[...] += sum(g[:, c] for c in chunks(g.shape[1], 128))

        lax.fori_loop(0, shapes[k][0] * (rows // 16), add, None)


def sum_of_squares(*pairs):
    n = 5
    arrays = [a for pair in pairs for a in pair[:2]]
    shapes = [(pair[2], *a.shape[1:]) for pair in pairs for a in pair[:2]]
    held = [pltpu.VMEM(shape, a.dtype) for shape, a in zip(shapes, arrays, strict=True)]
    return pl.pallas_call(
        functools.partial(squares_kernel, shapes=shapes, n=n),
        in_specs=[pl.BlockSpec(memory_space=pl.ANY)] * len(arrays),
        out_specs=pl.BlockSpec(memory_space=pltpu.VMEM),
        out_shape=out((8, 128), F32),
        scratch_shapes=[*held, pltpu.SemaphoreType.DMA((len(arrays), n))],
        compiler_params=params(),
        cost_estimate=cost(1e9, 4e6 * len(arrays)),
        name="squares",
    )(*arrays)


def updated(g, w, m, v):
    m = 0.9 * m + 0.1 * g
    v = 0.95 * v + 0.05 * g * g
    wide = w.astype(F32)
    return (wide - 0.02 * (m * lax.rsqrt(v + 1e-8) + 0.1 * wide)).astype(BF), m, v


def gradient(factor, keep, far, r):
    return (keep[r] + far[r].astype(F32)).astype(BF).astype(F32) * factor[0]


def adam_kernel(at, factor, keep, far, w, m, v, *rest, tails):
    w_out, m_out, v_out, w_new, *tail = rest[-4 - tails :]

    def rows(r):
        w_out[r], m_out[r], v_out[r] = updated(gradient(factor, keep, far, r), w[r], m[r], v[r])
        w_new[r] = w_out[r]

    cols = w.shape[1] // PIECES
    size = math.gcd(w.shape[0], 32)
    loop(w.shape[0] // size, size, lambda r: loop(PIECES, cols, lambda c: rows((r, c))))
    for o in tail:
        o[...] = w_out[:, w.shape[1] - o.shape[1] :]


def adam(at, factor, layer, which, part, keep, far, w, m, v, before, tail=0):
    rows, cols = keep.shape[1:]
    low, high, n = part
    br = rows // n
    own = pl.BlockSpec((None, br, cols), lambda i, at: (layer, low + i, 0))
    grad = pl.BlockSpec((None, br, cols), lambda i, at: (which, low + i, 0))
    there = pl.BlockSpec((None, br, cols), lambda i, at: (layer, (2 * at[0] + at[1]) * n + low + i, 0))
    return call(
        functools.partial(adam_kernel, tails=int(tail > 0)),
        at,
        (high - low,),
        [pl.BlockSpec(memory_space=pltpu.SMEM), grad, grad, there, own, own] + [pl.BlockSpec(memory_space=pl.ANY)] * len(before),
        [pl.BlockSpec((br, cols), lambda i, at: (i, 0)), own, own, there] + [pl.BlockSpec((br, tail), lambda i, at: (i, 0))] * (tail > 0),
        [out((br * (high - low), cols)), out(m.shape, F32), out(v.shape, F32), out(w.shape)] + [out((br * (high - low), tail))] * (tail > 0),
        [factor, keep, far, w, m, v, *before],
        1e9,
        6e6 * (high - low),
        input_output_aliases={7: 1, 8: 2, 9: 3} if before else {},
    )


def adam_far_kernel(at, factor, keep, far, w, *refs, start):
    *moments, before, w_out, w_new = refs
    first = at[2] == 0

    def update(crossed, handed):
        def rows(r):
            m, v = jnp.where(first, crossed[r, :], handed[r, :]), jnp.where(first, handed[r, :], crossed[r, :])
            w_out[r, :], _, _ = updated(gradient(factor, keep, far, (r, slice(None))), w[r, :], m, v)
            w_new[r, :] = w_out[r, :]

        loop(w.shape[0] // 32, 32, rows)

    if len(moments) == 2:
        update(*moments)
    else:
        early = pl.program_id(1) + start < EARLY
        pl.when(early)(lambda: update(*moments[:2]))
        pl.when(~early)(lambda: update(*moments[2:]))


def adam_far(at, factor, layer, which, start, count, keep, far, w, moments, before):
    rows, cols = keep.shape[1:]
    n = 2
    br, bc = rows // n, cols // PIECES
    grad = pl.BlockSpec((None, br, bc), lambda i, j, at: (which, i, j))
    flat = pl.BlockSpec((br, bc), lambda i, j, at: (i, j))
    there = pl.BlockSpec((None, br, bc), lambda i, j, at: (layer, (2 * (1 - at[0]) + at[1]) * n + i, j))
    early = pl.BlockSpec((br, bc), lambda i, j, at: (i, jnp.minimum(j + start, EARLY - 1)))
    late = pl.BlockSpec((br, bc), lambda i, j, at: (i, jnp.maximum(j + start - EARLY, 0)))
    specs = ([early] * 2 if start < EARLY else []) + ([late] * 2 if start + count > EARLY else [])
    moments = moments[: len(specs)]
    return call(
        functools.partial(adam_far_kernel, start=start),
        at,
        (n, count),
        [pl.BlockSpec(memory_space=pltpu.SMEM), grad, grad, there, *specs, pl.BlockSpec(memory_space=pl.ANY)],
        [flat, there],
        [out((rows, bc * count)), out(w.shape)],
        [factor, keep, far, w, *moments, before],
        1e9,
        30e6,
        input_output_aliases={5 + len(specs): 1},
    )


def place_kernel(at, *refs, count):
    for n in range(count):
        pl.when(pl.program_id(0) == n)(functools.partial(lambda n: refs[-1].__setitem__(..., refs[n][...]), n))


def place(at, layer, part, blocks, wheres, before, piece=None):
    low, high, n = part
    k = high - low
    rows, cols = blocks[0].shape
    br, bc = rows // k, cols if piece is None else before.shape[2] // PIECES
    m = cols // bc

    def spec(n):
        def index(i, j, l, at):
            return jnp.where(i < n, 0, jnp.where(i > n, k - 1, j)), jnp.where(i < n, 0, jnp.where(i > n, m - 1, l))

        return pl.BlockSpec((br, bc), index)

    def where(i, j, l, at):
        b = wheres[0](at)
        for k, w in enumerate(wheres[1:], 1):
            b = jnp.where(i == k, w(at), b)
        return layer, b * n + low + j, l + (piece or 0)

    return call(
        functools.partial(place_kernel, count=len(blocks)),
        at,
        (len(blocks), k, m),
        [spec(n) for n in range(len(blocks))] + [pl.BlockSpec(memory_space=pl.ANY)],
        pl.BlockSpec((None, br, bc), where),
        out(before.shape),
        [*blocks, before],
        1e9,
        1.2e6 * k * len(blocks),
        input_output_aliases={1 + len(blocks): 0},
    )


def after(value, *others):
    return lax.optimization_barrier((value, *others))[0]


ACROSS = [(0, 2), (2, 0), (1, 3), (3, 1)]
SIBLING = [(0, 1), (1, 0), (2, 3), (3, 2)]


def across(a):
    return lax.ppermute(a, "dp", ACROSS)


def sibling(a):
    return lax.ppermute(a, "dp", SIBLING)


def step(x, dy, w_gate, w_up, w_down, m_gate, m_up, m_down, v_gate, v_up, v_down):
    dp = lax.axis_index("dp")
    at = jnp.stack([dp // 2, dp % 2, lax.axis_index("rep")]).astype(jnp.int32)
    x, dy = x[0], dy[0]
    d, f = w_gate.shape[1:]

    def blocks(a):
        return a.reshape(4, a.shape[0] // 4, a.shape[1])

    dy_far = across(dy)
    moments = m_gate, v_gate, m_up, v_up
    a1, hid1, s1, q1, h1, early, late = first(at, x, w_gate, w_up, w_down, moments)
    h1_far = across(h1)

    def brought(half):
        crossed = across(half)
        return crossed, lax.ppermute(crossed, "rep", [(0, 1), (1, 0)])

    far_moments = (*brought(early), *brought(late))
    a2, dgu2, hid2, d1 = second(at, h1, dy, w_gate, w_up, w_down)

    dgu1, theirs = hidden_back(at, w_down, d1, s1, q1, blocks(a1))
    got_wide = sibling(theirs)
    pairs = [(blocks(hid1), after(d1, theirs))]
    (theirs,) = grad_tall(at, pairs, on(False, False), on(True, False), keeps=False)
    got_down = sibling(theirs)
    got_wide = after(got_wide, theirs)
    send, keep_wide1 = grad_wide(at, blocks(a1), dgu1, on(False, True), on(True, True), got_wide)
    far_wide1 = across(send)
    got_down = after(got_down, keep_wide1)
    send, keep_down1 = grad_tall(at, pairs, on(False, True), on(True, True), got_down)
    far_down1 = across(send)

    h1_far = after(h1_far, keep_down1)
    a2, dgu2, hid2f = second(at, h1_far, dy_far, w_gate, w_up, w_down, [a2, dgu2])
    send, keep_wide2 = grad_whole(at, a2, dgu2)
    far_wide2 = sibling(send)
    pairs = [(blocks(hid2), dy), (blocks(after(hid2f, keep_wide2)), dy_far)]
    send, keep_down2 = grad_tall(at, pairs, on(True, False), on(True, True))
    far_down2 = sibling(send)
    keep_down1, far_down1, keep_down2, far_down2 = (a[None] for a in (keep_down1, far_down1, keep_down2, far_down2))
    squares = sum_of_squares((keep_wide1, far_wide1, 2), (keep_down1, far_down1, 1), (keep_wide2, far_wide2, 2))
    far_down2 = after(far_down2, squares)
    squares = squares + sum_of_squares((keep_down2, far_down2, 1))
    squares = squares + sibling(squares)
    squares = squares + across(squares)
    factor = jnp.minimum(1.0, 0.5 * lax.rsqrt(jnp.sum(squares) / (6 * d * f) + 1e-30)).reshape(1)

    weights = {"gate": (w_gate, m_gate, v_gate), "up": (w_up, m_up, v_up), "down": (w_down, m_down, v_down)}
    grads = {
        "gate1": (1, 0, keep_wide2, far_wide2),
        "up1": (1, 1, keep_wide2, far_wide2),
        "down1": (1, 0, keep_down2, far_down2),
        "gate0": (0, 0, keep_wide1, far_wide1),
        "up0": (0, 1, keep_wide1, far_wide1),
        "down0": (0, 0, keep_down1, far_down1),
    }
    new = dict.fromkeys(weights, ())

    def update(which, part, tail=0):
        name = which[:-1]
        first, *rest = adam(at, factor, *grads[which][:2], part, *grads[which][2:], *weights[name], new[name], tail)
        new[name] = rest[:3]
        return first, *rest[3:]

    def put(which, part, *blocks, piece=None):
        name = which[:-1]
        *moments, w = new[name]
        where, arrays = zip(*blocks, strict=True)
        new[name] = [*moments, place(at, grads[which][0], part, arrays, where, w, piece)]

    def send(n):
        which, part = PARTS[n]
        (own,) = update(which, part)
        return across(own), sibling(own)

    def settle(sent):
        for n, (_, beside) in sent.items():
            put(*PARTS[n], (on(True, False), beside))
        for n, (away, _) in sent.items():
            put(*PARTS[n], (on(False, True), away))
            put(*PARTS[n], (on(False, False), sibling(away)))

    whole = (0, 2, 2)

    def update_far(name, which, count):
        *moments, w = new[name]
        arrays = keep_wide2, far_wide2, weights[name][0], far_moments
        away, w = adam_far(at, factor, 1, which, (which - 2) * PIECES, count, *arrays, w)
        new[name] = [*moments, w]
        return sibling(away)

    sent = {n: send(n) for n in range(len(PARTS) - 2)}
    (own,) = update("gate1", whole)
    last = update_far("gate", 2, PIECES)
    put("gate1", whole, (on(True, False), sibling(own)), (on(False, False), last))
    own, tail = update("up1", whole, f // PIECES * (PIECES - OF_UP))
    tail = across(tail)
    put("up1", whole, (on(True, False), sibling(own)))
    last = update_far("up", 3, OF_UP)
    put("up1", whole, (on(False, False), last), piece=0)
    settle(sent)
    put("up1", whole, (on(False, True), tail), (on(False, False), sibling(tail)), piece=OF_UP)
    settle({n: send(n) for n in range(len(sent), len(PARTS))})
    return tuple(new[name][i] for i in (2, 0, 1) for name in weights)


PARTS = [
    ("down1", (0, 1, 10)),
    ("down1", (1, 2, 10)),
    ("down1", (1, 2, 5)),
    ("down1", (2, 5, 5)),
    ("gate0", (0, 2, 2)),
    ("up0", (0, 2, 2)),
    ("down0", (0, 3, 5)),
    ("down0", (3, 5, 5)),
]


def solution(mesh):
    tokens, whole, rows = P(("rep", "dp")), P(), P(None, "dp")

    return jax.shard_map(
        step,
        mesh=mesh,
        in_specs=(tokens,) * 2 + (whole,) * 3 + (rows,) * 6,
        out_specs=(P("rep"),) * 3 + (P("rep", "dp"),) * 6,
        check_vma=False,
    )
```

```python
import functools
import math

import jax
import jax.numpy as jnp
from jax import lax
from jax.experimental import pallas as pl
from jax.experimental.pallas import tpu as pltpu
from jax.sharding import PartitionSpec as P

BF, F32 = jnp.bfloat16, jnp.float32
NN = (((1,), (0,)), ((), ()))
NT = (((1,), (1,)), ((), ()))
CHUNK = 256
TOKENS, UNITS = 1024, 512


def dot(a, b, dims):
    return lax.dot_general(a, b, dims, preferred_element_type=F32)


def params():
    return pltpu.CompilerParams(vmem_limit_bytes=67043328)


def cost(flops, nbytes):
    return pl.CostEstimate(flops=int(flops), bytes_accessed=int(nbytes), transcendentals=0)


def out(shape, dtype=BF):
    return jax.ShapeDtypeStruct(shape, dtype)


def once(shape, index):
    return pl.BlockSpec(shape, index, pipeline_mode=pl.Buffered(1))


def call(kernel, at, grid, in_specs, out_specs, out_shape, operands, flops, nbytes, scratch=(), **kw):
    return pl.pallas_call(
        kernel,
        grid_spec=pltpu.PrefetchScalarGridSpec(
            num_scalar_prefetch=1, grid=grid, in_specs=in_specs, out_specs=out_specs, scratch_shapes=scratch
        ),
        out_shape=out_shape,
        compiler_params=params(),
        cost_estimate=cost(flops, nbytes),
        **kw,
    )(at, *operands)


def sigmoid(x):
    return 0.5 * jnp.tanh(0.5 * x) + 0.5


def chunks(n, size=CHUNK):
    return [slice(at, min(at + size, n)) for at in range(0, n, size)]


def loop(n, size, body):
    lax.fori_loop(0, n, lambda i, _: body(pl.ds(pl.multiple_of(i * size, size), size)), None)


def norm(h, a, a_out):
    def rows(r):
        wide = h[r, :].astype(F32)
        scale = lax.rsqrt(jnp.mean(wide * wide, -1, keepdims=True) + 1e-6)
        a[r, :] = (wide * scale).astype(BF)
        a_out[:, r] = a[r, :].T

    loop(a.shape[0] // CHUNK, CHUNK, rows)


def unless_first(total):
    return jnp.where(pl.program_id(1) == 0, 0.0, total)


def only(a, n, axis):
    return jnp.where(lax.broadcasted_iota(jnp.int32, a.shape, axis) < n, a, jnp.zeros_like(a))


PIECES, OF_UP, EARLY = 5, 2, 6


def copied(at, step, moments, early, late, held, in_sems, out_sems):
    cols = held.shape[2]
    n = PIECES + OF_UP

    def columns(block):
        return pl.ds(pl.multiple_of(block * cols, 128), cols)

    def came_in(p):
        return pltpu.make_async_copy(moments[0].at[1, :, columns(0)], held.at[p % 2], in_sems.at[p % 2])

    def went_out(p):
        return pltpu.make_async_copy(held.at[p % 2], early.at[:, columns(0)], out_sems.at[p % 2])

    pl.when((step >= 2) & (step < n + 2))(lambda: went_out(step).wait())
    for which in range(2):
        for rep in range(2):

            @pl.when((step >= which * PIECES) & (step < min((which + 1) * PIECES, n)) & (at[2] == rep))
            def _(source=moments[2 * which + rep], block=step - which * PIECES):
                pltpu.make_async_copy(source.at[1, :, columns(block)], held.at[step % 2], in_sems.at[step % 2]).start()

    before = step - 1
    pl.when((before >= 0) & (before < n))(lambda: came_in(before).wait())
    for low, high, target in ((0, EARLY, early), (EARLY, n, late)):

        @pl.when((before >= low) & (before < high))
        def _(target=target, block=before - low):
            pltpu.make_async_copy(held.at[before % 2], target.at[:, columns(block)], out_sems.at[before % 2]).start()


def first_kernel(at, x, wg, wu, wd, *refs, f):
    moments, (a_out, hid, s_out, q_out, h_out, early, late, a, units, total, *held) = refs[:4], refs[4:]
    i, j = pl.program_id(0), pl.program_id(1)
    left = f - j * UNITS
    copied(at, i * pl.num_programs(1) + j, moments, early, late, *held)

    @pl.when(j == 0)
    def _():
        norm(x, a, a_out)

    for c in chunks(UNITS):
        for r in chunks(a.shape[0]):
            gate, up = dot(a[r, :], wg[:, c], NN), dot(a[r, :], wu[:, c], NN)
            sig = sigmoid(gate)
            silu = gate * sig
            units[r, c] = only((silu * up).astype(BF), left - c.start, 1)
            hid[c, r] = units[r, c].T
            s_out[r, c] = silu
            q_out[r, c] = up * (sig + silu * (1 - sig))
    for c in chunks(total.shape[1]):
        total[:, c] = unless_first(total[:, c]) + dot(units[...], only(wd[:, c], left, 0), NN)

    @pl.when(j == pl.num_programs(1) - 1)
    def _():
        def rows(r):
            h_out[r, :] = x[r, :] + total[r, :].astype(BF)

        loop(x.shape[0] // CHUNK, CHUNK, rows)


def first(at, x, w_gate, w_up, w_down, moments):
    m = moments[0]
    t, d = x.shape
    f = w_gate.shape[2]
    n = pl.cdiv(f, UNITS)
    wide = pl.BlockSpec((None, TOKENS, UNITS), lambda i, j, at: (j, i, 0))
    weight = pl.BlockSpec((None, d, UNITS), lambda i, j, at: (0, 0, j))
    state = pl.BlockSpec((TOKENS, d), lambda i, j, at: (i, 0))
    return call(
        functools.partial(first_kernel, f=f),
        at,
        (t // TOKENS, pl.cdiv(f, UNITS)),
        [state, weight, weight, pl.BlockSpec((None, UNITS, d), lambda i, j, at: (0, j, 0))]
        + [pl.BlockSpec(memory_space=pl.ANY)] * 4,
        [
            pl.BlockSpec((d, TOKENS), lambda i, j, at: (0, i)),
            pl.BlockSpec((UNITS, TOKENS), lambda i, j, at: (j, i)),
            wide,
            wide,
            state,
        ]
        + [pl.BlockSpec(memory_space=pl.ANY)] * 2,
        [out((d, t)), out((f, t)), *[out((n, t, UNITS), F32)] * 2, out((t, d))]
        + [out((m.shape[1], n * f // PIECES), F32) for n in (EARLY, PIECES + OF_UP - EARLY)],
        (x, w_gate, w_up, w_down, *moments),
        6 * t * d * f,
        190e6,
        scratch=[
            pltpu.VMEM((TOKENS, d), BF),
            pltpu.VMEM((TOKENS, UNITS), BF),
            pltpu.VMEM((TOKENS, d), F32),
            pltpu.VMEM((2, m.shape[1], f // PIECES), F32),
            pltpu.SemaphoreType.DMA((2,)),
            pltpu.SemaphoreType.DMA((2,)),
        ],
    )


def second_units(a, dy, wg, wu, wd, hid, dgu, left):
    for c in chunks(hid.shape[0]):
        for r in chunks(a.shape[0]):
            gate, up = dot(a[r, :], wg[:, c], NN), dot(a[r, :], wu[:, c], NN)
            back = dot(dy[r, :], wd[c, :], NT).astype(BF).astype(F32)
            sig = sigmoid(gate)
            silu = gate * sig
            hid[c, r] = (silu * up).astype(BF).T
            dgu[0, r, c] = only((back * (up * (sig + silu * (1 - sig)))).astype(BF), left - c.start, 1)
            dgu[1, r, c] = only((back * silu).astype(BF), left - c.start, 1)


def second_kernel(at, h, dy, wg, wu, wd, a_before, dgu_before, a_out, dgu, hid, a, *, f):
    j = pl.program_id(1)

    @pl.when(j == 0)
    def _():
        norm(h, a, a_out)

    second_units(a, dy, wg, wu, wd, hid, dgu, f - j * hid.shape[0])


def second_back_kernel(at, h, dy, wg, wu, wd, a_out, dgu, hid, d_out, a, of_gate, of_up, *, f):
    j = pl.program_id(1)
    left = f - j * UNITS

    @pl.when(j == 0)
    def _():
        norm(h, a, a_out)

    second_units(a, dy, wg, wu, wd, hid, dgu, left)
    for c in chunks(of_gate.shape[1]):
        of_gate[:, c] = unless_first(of_gate[:, c]) + dot(dgu[0], only(wg[c, :], left, 1), NT)
        of_up[:, c] = unless_first(of_up[:, c]) + dot(dgu[1], only(wu[c, :], left, 1), NT)

    @pl.when(j == pl.num_programs(1) - 1)
    def _():
        def rows(r):
            da = (of_gate[r, :].astype(BF) + of_up[r, :].astype(BF)).astype(F32)
            wide = h[r, :].astype(F32)
            scale = lax.rsqrt(jnp.mean(wide * wide, -1, keepdims=True) + 1e-6)
            along = jnp.mean(da * wide, -1, keepdims=True) * (scale * scale * scale)
            d_out[r, :] = dy[r, :] + (da * scale - wide * along).astype(BF)

        loop(h.shape[0] // CHUNK, CHUNK, rows)


def second(at, h, dy, w_gate, w_up, w_down, before=None):
    t, d = h.shape
    f = w_gate.shape[2]
    far = before is not None
    bt, bf = TOKENS, UNITS
    weight = pl.BlockSpec((None, d, bf), lambda i, j, at: (1, 0, j))
    state = pl.BlockSpec((bt, d), lambda i, j, at: (i, 0))
    which = (lambda at: 1 - at[0]) if far else (lambda at: at[0])
    in_specs = [state, state, weight, weight, pl.BlockSpec((None, bf, d), lambda i, j, at: (1, j, 0))]
    out_specs = [
        pl.BlockSpec((None, d, bt), lambda i, j, at: (which(at), 0, i)),
        pl.BlockSpec((None, 2, bt, bf), lambda i, j, at: (which(at), 0, i, j)),
        pl.BlockSpec((bf, bt), lambda i, j, at: (j, i)),
    ]
    shapes = [out((2, d, t)), out((2, 2, t, f)), out((f, t))]
    scratch = [pltpu.VMEM((bt, d), BF)]
    operands = [h, dy, w_gate, w_up, w_down]
    aliases = {}
    if far:
        aliases = {6: 0, 7: 1}
        in_specs += [pl.BlockSpec(memory_space=pl.ANY)] * 2
        operands += before
    else:
        out_specs.append(state)
        shapes.append(out((t, d)))
        scratch += [pltpu.VMEM((bt, d), F32)] * 2
    return pl.pallas_call(
        functools.partial(second_kernel if far else second_back_kernel, f=f),
        grid_spec=pltpu.PrefetchScalarGridSpec(
            num_scalar_prefetch=1,
            grid=(t // bt, pl.cdiv(f, bf)),
            in_specs=in_specs,
            out_specs=out_specs,
            scratch_shapes=scratch,
        ),
        out_shape=shapes,
        input_output_aliases=aliases,
        compiler_params=params(),
        cost_estimate=cost((6 if far else 10) * t * d * f, 130e6),
        name="second" if far else "second_back",
    )(at, *operands)


def on(x_same, core_same):
    def block(at):
        return 2 * (at[0] if x_same else 1 - at[0]) + (at[1] if core_same else 1 - at[1])

    return block


def hidden_back_kernel(at, w, d, s, q, one, two, dgu, theirs):
    for r in chunks(d.shape[0]):
        back = dot(d[r, :], w[...], NT).astype(BF).astype(F32)
        dgu[1, r, :] = (back * s[r, :]).astype(BF)
        dgu[0, r, :] = (back * q[r, :]).astype(BF)
    left = jnp.concatenate([one[...], two[...]], 0)
    for which in range(2):
        theirs[which] = dot(left, dgu[which], NN).reshape(theirs.shape[1:]).astype(BF)


def hidden_back(at, w_down, d_h, s, q, a):
    t, d = d_h.shape
    f = w_down.shape[1]
    rows, bf = a.shape[1], UNITS
    wide = pl.BlockSpec((None, t, bf), lambda j, at: (j, 0, 0))
    return call(
        hidden_back_kernel,
        at,
        (pl.cdiv(f, bf),),
        [
            pl.BlockSpec((None, bf, d), lambda j, at: (0, j, 0)),
            once((t, d), lambda j, at: (0, 0)),
            wide,
            wide,
            once((None, rows, t), lambda j, at: (on(False, False)(at), 0, 0)),
            once((None, rows, t), lambda j, at: (on(True, False)(at), 0, 0)),
        ],
        [pl.BlockSpec((2, t, bf), lambda j, at: (0, 0, j)), pl.BlockSpec((2, 2, rows, bf), lambda j, at: (0, 0, 0, j))],
        [out((2, t, f)), out((2, 2, rows, f))],
        (w_down, d_h, s, q, a, a),
        4 * t * d * f,
        160e6,
    )


def wide_kernel(at, one, two, right, got, send, keep):
    rows = one.shape[0]
    total = dot(jnp.concatenate([one[...], two[...]], 0), right[...], NN)
    total = total + got[...].reshape(total.shape).astype(F32)
    send[...], keep[...] = total[:rows].astype(BF), total[rows:]


def grad_wide(at, left, right, one, two, got):
    rows, t = left.shape[1:]
    f = right.shape[2]
    bn = 1536
    return call(
        wide_kernel,
        at,
        (2, pl.cdiv(f, bn)),
        [once((None, rows, t), lambda w, j, at, b=b: (b(at), 0, 0)) for b in (one, two)]
        + [pl.BlockSpec((None, t, bn), lambda w, j, at: (w, 0, j)), pl.BlockSpec((None, 2, rows, bn), lambda w, j, at: (w, 0, 0, j))],
        [pl.BlockSpec((None, rows, bn), lambda w, j, at: (w, 0, j))] * 2,
        [out((2, rows, f)), out((2, rows, f), F32)],
        (left, left, right, got),
        8 * rows * t * f,
        60e6,
    )


def whole_kernel(at, which, left0, left1, right0, right1, send, keep, total):
    needed = (pl.program_id(0) == 0) | (pl.program_id(1) < which[1])

    @pl.when(needed)
    def _():
        total[...] = (dot(left0[...], right0[...], NN) + dot(left1[...], right1[...], NN)).reshape(total.shape)
        send[...], keep[...] = total[1 - at[1]].astype(BF), total[at[1]]

    @pl.when(~needed)
    def _():
        send[...], keep[...] = jnp.zeros_like(send), jnp.zeros_like(keep)


def grad_whole(at, left, right, x, pieces):
    d, t = left.shape[1:]
    f = right.shape[3]
    rows, bn = d // 4, 768
    same = pl.BlockSpec((None, rows, bn), lambda w, j, at, which: (w, 0, j))
    which = jnp.stack([x, jnp.full((), pl.cdiv(f * pieces // PIECES, bn), x.dtype)])
    return pl.pallas_call(
        whole_kernel,
        grid_spec=pltpu.PrefetchScalarGridSpec(
            num_scalar_prefetch=2,
            grid=(2, pl.cdiv(f, bn)),
            in_specs=[pl.BlockSpec((None, 2 * rows, t), lambda w, j, at, which, x=x: (x, which[0], 0)) for x in range(2)]
            + [pl.BlockSpec((None, None, t, bn), lambda w, j, at, which, x=x: (x, w, 0, j)) for x in range(2)],
            out_specs=[same, same],
            scratch_shapes=[pltpu.VMEM((2, rows, bn), F32)],
        ),
        out_shape=[out((2, rows, f)), out((2, rows, f), F32)],
        compiler_params=params(),
        cost_estimate=cost(4 * d * t * f, 80e6),
        name="grad_whole",
    )(at, which, left, left, right, right)


def tall_kernel(at, *refs, terms, add, keeps):
    operands, rest = refs[: 2 * terms], refs[2 * terms :]
    half = pl.num_programs(0) // 2
    total = 0
    for left, right in zip(operands[::2], operands[1::2], strict=True):
        total = total + dot(left[...], right[...], NN)
    if add:
        total = total + rest[0][...].astype(F32)
    if not keeps:
        rest[-1][...] = total.astype(BF)
        return

    @pl.when(pl.program_id(0) < half)
    def _():
        rest[-2][...] = total.astype(BF)

    @pl.when(pl.program_id(0) >= half)
    def _():
        rest[-1][...] = total


def grad_tall(at, pairs, one, two, got=None, keeps=True, half=4):
    rows, t = pairs[0][0].shape[1:]
    d = pairs[0][1].shape[1]
    bm = rows // half
    in_specs, operands = [], []
    for left, right in pairs:
        in_specs += [
            pl.BlockSpec((None, bm, t), lambda j, at: (jnp.where(j < half, one(at), two(at)), j % half, 0)),
            once(right.shape, lambda j, at: (0, 0)),
        ]
        operands += [left, right]
    if got is not None:
        in_specs.append(pl.BlockSpec((None, bm, d), lambda j, at: (j // half, j % half, 0)))
        operands.append(got)
    if keeps:
        out_specs = [pl.BlockSpec((bm, d), lambda j, at: (jnp.minimum(j, half - 1), 0)), pl.BlockSpec((bm, d), lambda j, at: (jnp.maximum(j - half, 0), 0))]
        shapes = [out((rows, d)), out((rows, d), F32)]
    else:
        out_specs = [pl.BlockSpec((None, bm, d), lambda j, at: (j // half, j % half, 0))]
        shapes = [out((2, rows, d))]
    return call(
        functools.partial(tall_kernel, terms=len(pairs), add=got is not None, keeps=keeps),
        at,
        (2 * half,),
        in_specs,
        out_specs,
        shapes,
        operands,
        4 * rows * t * d * len(pairs),
        60e6,
    )


def squares_kernel(*refs, shapes, n):
    arrays, o, held, sems = refs[: len(shapes)], refs[len(shapes)], refs[len(shapes) + 1 : -1], refs[-1]

    def copies(k, i):
        rows = shapes[k][1] // n
        r = pl.ds(i * rows, rows)
        return pltpu.make_async_copy(arrays[k].at[pl.ds(0, shapes[k][0]), r], held[k].at[:, r], sems.at[k, i])

    everything = [(k, i) for k in range(0, len(shapes), 2) for i in range(n)]
    for k, i in everything:
        copies(k, i).start()
        copies(k + 1, i).start()
    o[...] = jnp.zeros_like(o)
    for k, i in everything:
        copies(k, i).wait()
        copies(k + 1, i).wait()
        rows = shapes[k][1] // n

        def add(t, _, k=k, start=i * rows, size=rows // 16):
            r = pl.ds(pl.multiple_of(start + t % size * 16, 16), 16)
            g = (held[k][t // size, r, :] + held[k + 1][t // size, r, :].astype(F32)).astype(BF).astype(F32)
            g = jnp.sum((g * g).reshape(-1, 8, g.shape[-1]), 0)
            o[...] += sum(g[:, c] for c in chunks(g.shape[1], 128))

        lax.fori_loop(0, shapes[k][0] * (rows // 16), add, None)


def sum_of_squares(*pairs):
    n = 5
    arrays = [a for pair in pairs for a in pair[:2]]
    shapes = [(pair[2], *a.shape[1:]) for pair in pairs for a in pair[:2]]
    held = [pltpu.VMEM(shape, a.dtype) for shape, a in zip(shapes, arrays, strict=True)]
    return pl.pallas_call(
        functools.partial(squares_kernel, shapes=shapes, n=n),
        in_specs=[pl.BlockSpec(memory_space=pl.ANY)] * len(arrays),
        out_specs=pl.BlockSpec(memory_space=pltpu.VMEM),
        out_shape=out((8, 128), F32),
        scratch_shapes=[*held, pltpu.SemaphoreType.DMA((len(arrays), n))],
        compiler_params=params(),
        cost_estimate=cost(1e9, 4e6 * len(arrays)),
        name="squares",
    )(*arrays)


def updated(g, w, m, v):
    m = 0.9 * m + 0.1 * g
    v = 0.95 * v + 0.05 * g * g
    wide = w.astype(F32)
    return (wide - 0.02 * (m * lax.rsqrt(v + 1e-8) + 0.1 * wide)).astype(BF), m, v


def gradient(factor, keep, far, r):
    return (keep[r] + far[r].astype(F32)).astype(BF).astype(F32) * factor[0]


def adam_kernel(at, factor, keep, far, w, m, v, *rest, tails):
    w_out, m_out, v_out, w_new, *tail = rest[-4 - tails :]

    def rows(r):
        w_out[r], m_out[r], v_out[r] = updated(gradient(factor, keep, far, r), w[r], m[r], v[r])
        w_new[r] = w_out[r]

    cols = w.shape[1] // (PIECES if w.shape[1] > 2048 else 1)
    size = math.gcd(w.shape[0], 32)
    loop(w.shape[0] // size, size, lambda r: loop(w.shape[1] // cols, cols, lambda c: rows((r, c))))
    for o in tail:
        o[...] = w_out[:, w.shape[1] - o.shape[1] :]


def adam(at, factor, layer, which, part, keep, far, w, m, v, before, tail=0):
    rows, cols = keep.shape[1:]
    low, high, n = part
    br = rows // n
    own = pl.BlockSpec((None, br, cols), lambda i, at: (layer, low + i, 0))
    grad = pl.BlockSpec((None, br, cols), lambda i, at: (which, low + i, 0))
    there = pl.BlockSpec((None, br, cols), lambda i, at: (layer, (2 * at[0] + at[1]) * n + low + i, 0))
    return call(
        functools.partial(adam_kernel, tails=int(tail > 0)),
        at,
        (high - low,),
        [pl.BlockSpec(memory_space=pltpu.SMEM), grad, grad, there, own, own] + [pl.BlockSpec(memory_space=pl.ANY)] * len(before),
        [pl.BlockSpec((br, cols), lambda i, at: (i, 0)), own, own, there] + [pl.BlockSpec((br, tail), lambda i, at: (i, 0))] * (tail > 0),
        [out((br * (high - low), cols)), out(m.shape, F32), out(v.shape, F32), out(w.shape)] + [out((br * (high - low), tail))] * (tail > 0),
        [factor, keep, far, w, m, v, *before],
        1e9,
        6e6 * (high - low),
        input_output_aliases={7: 1, 8: 2, 9: 3} if before else {},
    )


def adam_far_kernel(at, factor, keep, far, w, *refs, start):
    *moments, before, w_out, w_new = refs
    first = at[2] == 0

    def update(crossed, handed):
        def rows(r):
            m, v = jnp.where(first, crossed[r, :], handed[r, :]), jnp.where(first, handed[r, :], crossed[r, :])
            w_out[r, :], _, _ = updated(gradient(factor, keep, far, (r, slice(None))), w[r, :], m, v)
            w_new[r, :] = w_out[r, :]

        loop(w.shape[0] // 32, 32, rows)

    if len(moments) == 2:
        update(*moments)
    else:
        early = pl.program_id(1) + start < EARLY
        pl.when(early)(lambda: update(*moments[:2]))
        pl.when(~early)(lambda: update(*moments[2:]))


def adam_far(at, factor, layer, which, start, count, keep, far, w, moments, before):
    rows, cols = keep.shape[1:]
    n = 2
    br, bc = rows // n, cols // PIECES
    grad = pl.BlockSpec((None, br, bc), lambda i, j, at: (which, i, j))
    flat = pl.BlockSpec((br, bc), lambda i, j, at: (i, j))
    there = pl.BlockSpec((None, br, bc), lambda i, j, at: (layer, (2 * (1 - at[0]) + at[1]) * n + i, j))
    early = pl.BlockSpec((br, bc), lambda i, j, at: (i, jnp.minimum(j + start, EARLY - 1)))
    late = pl.BlockSpec((br, bc), lambda i, j, at: (i, jnp.maximum(j + start - EARLY, 0)))
    specs = ([early] * 2 if start < EARLY else []) + ([late] * 2 if start + count > EARLY else [])
    moments = moments[: len(specs)]
    return call(
        functools.partial(adam_far_kernel, start=start),
        at,
        (n, count),
        [pl.BlockSpec(memory_space=pltpu.SMEM), grad, grad, there, *specs, pl.BlockSpec(memory_space=pl.ANY)],
        [flat, there],
        [out((rows, bc * count)), out(w.shape)],
        [factor, keep, far, w, *moments, before],
        1e9,
        30e6,
        input_output_aliases={5 + len(specs): 1},
    )


def place_kernel(at, *refs, count):
    for n in range(count):
        pl.when(pl.program_id(0) == n)(functools.partial(lambda n: refs[-1].__setitem__(..., refs[n][...]), n))


def place(at, layer, part, blocks, wheres, before, piece=None):
    low, high, n = part
    k = high - low
    rows, cols = blocks[0].shape
    br, bc = rows // k, cols if piece is None else before.shape[2] // PIECES
    m = cols // bc

    def spec(n):
        def index(i, j, l, at):
            return jnp.where(i < n, 0, jnp.where(i > n, k - 1, j)), jnp.where(i < n, 0, jnp.where(i > n, m - 1, l))

        return pl.BlockSpec((br, bc), index)

    def where(i, j, l, at):
        b = wheres[0](at)
        for k, w in enumerate(wheres[1:], 1):
            b = jnp.where(i == k, w(at), b)
        return layer, b * n + low + j, l + (piece or 0)

    return call(
        functools.partial(place_kernel, count=len(blocks)),
        at,
        (len(blocks), k, m),
        [spec(n) for n in range(len(blocks))] + [pl.BlockSpec(memory_space=pl.ANY)],
        pl.BlockSpec((None, br, bc), where),
        out(before.shape),
        [*blocks, before],
        1e9,
        1.2e6 * k * len(blocks),
        input_output_aliases={1 + len(blocks): 0},
    )


def after(value, *others):
    return lax.optimization_barrier((value, *others))[0]


ACROSS = [(0, 2), (2, 0), (1, 3), (3, 1)]
SIBLING = [(0, 1), (1, 0), (2, 3), (3, 2)]


def across(a):
    return lax.ppermute(a, "dp", ACROSS)


def sibling(a):
    return lax.ppermute(a, "dp", SIBLING)


def step(x, dy, w_gate, w_up, w_down, m_gate, m_up, m_down, v_gate, v_up, v_down):
    dp = lax.axis_index("dp")
    at = jnp.stack([dp // 2, dp % 2, lax.axis_index("rep")]).astype(jnp.int32)
    x, dy = x[0], dy[0]
    d, f = w_gate.shape[1:]

    def blocks(a):
        return a.reshape(4, a.shape[0] // 4, a.shape[1])

    dy_far = across(dy)
    moments = m_gate, v_gate, m_up, v_up
    a1, hid1, s1, q1, h1, early, late = first(at, x, w_gate, w_up, w_down, moments)
    h1_far = across(h1)

    def brought(half):
        crossed = across(half)
        return crossed, lax.ppermute(crossed, "rep", [(0, 1), (1, 0)])

    far_moments = (*brought(early), *brought(late))
    a2, dgu2, hid2, d1 = second(at, h1, dy, w_gate, w_up, w_down)

    dgu1, theirs = hidden_back(at, w_down, d1, s1, q1, blocks(a1))
    got_wide = sibling(theirs)
    pairs = [(blocks(hid1), after(d1, theirs))]
    (theirs,) = grad_tall(at, pairs, on(False, False), on(True, False), keeps=False)
    got_down = sibling(theirs)
    got_wide = after(got_wide, theirs)
    send, keep_wide1 = grad_wide(at, blocks(a1), dgu1, on(False, True), on(True, True), got_wide)
    far_wide1 = across(send)
    got_down = after(got_down, keep_wide1)
    send, keep_down1 = grad_tall(at, pairs, on(False, True), on(True, True), got_down)
    far_down1 = across(send)

    h1_far = after(h1_far, keep_down1)
    a2, dgu2, hid2f = second(at, h1_far, dy_far, w_gate, w_up, w_down, [a2, dgu2])
    send, keep_wide2 = grad_whole(at, a2, dgu2, at[0], PIECES)
    far_wide2 = sibling(send)
    pairs = [(blocks(hid2), dy), (blocks(after(hid2f, keep_wide2)), dy_far)]
    send, keep_down2 = grad_tall(at, pairs, on(True, False), on(True, True))
    far_down2 = sibling(send)
    keep_down1, far_down1, keep_down2, far_down2 = (a[None] for a in (keep_down1, far_down1, keep_down2, far_down2))
    squares = sum_of_squares((keep_wide1, far_wide1, 2), (keep_down1, far_down1, 1), (keep_wide2, far_wide2, 2))
    far_down2 = after(far_down2, squares)
    squares = squares + sum_of_squares((keep_down2, far_down2, 1))
    squares = squares + sibling(squares)
    squares = squares + across(squares)
    factor = jnp.minimum(1.0, 0.5 * lax.rsqrt(jnp.sum(squares) / (6 * d * f) + 1e-30)).reshape(1)

    weights = {"gate": (w_gate, m_gate, v_gate), "up": (w_up, m_up, v_up), "down": (w_down, m_down, v_down)}
    grads = {
        "gate1": (1, 0, keep_wide2, far_wide2),
        "up1": (1, 1, keep_wide2, far_wide2),
        "down1": (1, 0, keep_down2, far_down2),
        "gate0": (0, 0, keep_wide1, far_wide1),
        "up0": (0, 1, keep_wide1, far_wide1),
        "down0": (0, 0, keep_down1, far_down1),
    }
    new = dict.fromkeys(weights, ())

    def update(which, part, tail=0):
        name = which[:-1]
        first, *rest = adam(at, factor, *grads[which][:2], part, *grads[which][2:], *weights[name], new[name], tail)
        new[name] = rest[:3]
        return first, *rest[3:]

    def put(which, part, *blocks, piece=None):
        name = which[:-1]
        *moments, w = new[name]
        where, arrays = zip(*blocks, strict=True)
        new[name] = [*moments, place(at, grads[which][0], part, arrays, where, w, piece)]

    def send(n):
        which, part = PARTS[n]
        (own,) = update(which, part)
        return across(own), sibling(own)

    def settle(sent):
        for n, (_, beside) in sent.items():
            put(*PARTS[n], (on(True, False), beside))
        for n, (away, _) in sent.items():
            put(*PARTS[n], (on(False, True), away))
            put(*PARTS[n], (on(False, False), sibling(away)))

    whole = (0, 2, 2)

    def update_far(name, which, count):
        *moments, w = new[name]
        arrays = keep_other, far_other, weights[name][0], far_moments
        away, w = adam_far(at, factor, 1, which, which * PIECES, count, *arrays, w)
        new[name] = [*moments, w]
        return sibling(away)

    sent = {n: send(n) for n in range(len(PARTS) - 2)}
    send_other, keep_other = grad_whole(at, a2, dgu2, 1 - at[0], OF_UP)
    far_other = sibling(send_other)
    (own,) = update("gate1", whole)
    last = update_far("gate", 0, PIECES)
    put("gate1", whole, (on(True, False), sibling(own)), (on(False, False), last))
    own, tail = update("up1", whole, f // PIECES * (PIECES - OF_UP))
    tail = across(tail)
    put("up1", whole, (on(True, False), sibling(own)))
    last = update_far("up", 1, OF_UP)
    put("up1", whole, (on(False, False), last), piece=0)
    settle(sent)
    put("up1", whole, (on(False, True), tail), (on(False, False), sibling(tail)), piece=OF_UP)
    settle({n: send(n) for n in range(len(sent), len(PARTS))})
    return tuple(new[name][i] for i in (2, 0, 1) for name in weights)


PARTS = [
    ("down1", (0, 1, 10)),
    ("down1", (1, 2, 10)),
    ("down1", (1, 2, 5)),
    ("down1", (2, 5, 5)),
    ("gate0", (0, 2, 2)),
    ("up0", (0, 2, 2)),
    ("down0", (0, 3, 5)),
    ("down0", (3, 5, 5)),
]


def solution(mesh):
    tokens, whole, rows = P(("rep", "dp")), P(), P(None, "dp")

    return jax.shard_map(
        step,
        mesh=mesh,
        in_specs=(tokens,) * 2 + (whole,) * 3 + (rows,) * 6,
        out_specs=(P("rep"),) * 3 + (P("rep", "dp"),) * 6,
        check_vma=False,
    )
```
